32 devices in a mesh: dp: 2 (over x), row: 4 (over y, core), col: 4 (over z).
Axes of the slice: x: 2, y: 2, z: 4, core: 2. Of those that a mesh axis runs over, the one named last changes fastest.
Arguments:
- latents: float32 [24, 32, 128], P(('dp', 'row')), may hold values from -6 to 6
- labels: int32 [24], P(('dp', 'row')), may hold values from 0 to 999
- step_index: int32 [24], P(('dp', 'row')), may hold values from 1 to 8
- seeds: int32 [24], P(('dp', 'row')), may hold values from 0 to 2147483646
- class_table: bfloat16 [1000, 1152], replicated, may hold values from -6 to 6
- teacher_patch: bfloat16 [16, 1152], replicated, may hold values from -1.5 to 1.5
- teacher_mod: bfloat16 [1152, 3, 1152], P(('dp', 'row'), None, 'col'), may hold values from -0.1875 to 0.1875
- teacher_up: bfloat16 [1152, 4608], P(('dp', 'row'), 'col'), may hold values from -0.1875 to 0.1875
- teacher_down: bfloat16 [1152, 4608], P(('dp', 'row'), 'col'), may hold values from -0.09375 to 0.09375
- teacher_out: bfloat16 [16, 1152], replicated, may hold values from -0.1875 to 0.1875
- student_patch: bfloat16 [16, 1152], replicated, may hold values from -1.5 to 1.5
- student_mod: bfloat16 [1152, 3, 1152], P(('dp', 'row'), None, 'col'), may hold values from -0.1875 to 0.1875
- student_up: bfloat16 [1152, 4608], P(('dp', 'row'), 'col'), may hold values from -0.1875 to 0.1875
- student_down: bfloat16 [1152, 4608], P(('dp', 'row'), 'col'), may hold values from -0.09375 to 0.09375
- student_out: bfloat16 [16, 1152], replicated, may hold values from -0.1875 to 0.1875
Outputs:
- up_gradient: float32 [1152, 4608], P(('dp', 'row'), 'col')
- down_gradient: float32 [1152, 4608], P(('dp', 'row'), 'col')
The draws below stay inside these ranges and needn't reach their ends.
All inputs are finite; a program needn't handle non-finite values.
Results may differ from the reference program's by a relative error of at most 0.002.
Values may be sent and summed in bfloat16 or wider, within the bound.
No kernel may reach another device: no remote copies, remote signals or barrier semaphores. Data moves between devices by JAX's collectives and lax.ppermute only.
A program may use at most 128 MiB of HBM per device.

```python
import math
import jax
import jax.numpy as jnp
from jax import lax

D = 1152
FF = 4608
CLASSES = 1000
SEQ = 256
PATCH = 16
STEPS = 8
BATCH = 24
N_COL = 4


def touch_ends(values, own_key, smallest, high):
    shape = values.shape
    spot = [jax.random.randint(jax.random.fold_in(own_key, axis), (), 0, shape[axis]) for axis in range(len(shape))]
    values = values.at[tuple(spot)].set(smallest)
    longest = shape.index(max(shape))
    spot[longest] = (spot[longest] + 1) % shape[longest]
    return values.at[tuple(spot)].set(high)


def levels(own_key, shape, shards, least, high):
    gain, own = 1.0, jax.random.fold_in(own_key, 6)
    for dim, shards_of in shards:
        draws = jnp.exp(jax.random.uniform(jax.random.fold_in(own, dim), (shards_of,), jnp.float32, least / len(shards), high / len(shards)))
        gain = gain * jnp.repeat(draws, shape[dim] // shards_of).reshape([-1 if axis == dim else 1 for axis in range(len(shape))])
    return gain


def gaussian(stream_key, shape, deviation, reach, split=(), held_as=jnp.bfloat16):
    entries = deviation * jax.random.normal(stream_key, shape, jnp.float32)
    if split:
        entries = entries * levels(stream_key, shape, split, -0.22, 0.18)
    return jnp.clip(entries, -reach, reach).astype(held_as)


def setup_inputs(seed: int = 0) -> dict:
    streams_of = jax.random.split(jax.random.key(seed), 16)
    return {
        "latents": gaussian(streams_of[0], (BATCH, SEQ * PATCH // 128, 128), 1.0, 6.0, ((0, 8),), jnp.float32),
        "labels": touch_ends(jax.random.randint(streams_of[1], (BATCH,), 0, CLASSES), jax.random.fold_in(streams_of[1], 1), 0, CLASSES - 1).astype(jnp.int32),
        "step_index": touch_ends(jax.random.randint(streams_of[2], (BATCH,), 1, STEPS + 1), jax.random.fold_in(streams_of[2], 1), 1, STEPS).astype(jnp.int32),
        "seeds": touch_ends(jax.random.randint(streams_of[3], (BATCH,), 0, 2147483647), jax.random.fold_in(streams_of[3], 1), 0, 2147483646).astype(jnp.int32),
        "class_table": gaussian(streams_of[4], (CLASSES, D), 1.0, 6.0),
        "teacher_patch": gaussian(streams_of[5], (PATCH, D), PATCH ** -0.5, 1.5),
        "teacher_mod": gaussian(streams_of[6], (D, 3, D), D ** -0.5, 0.1875, ((0, 8), (2, 4))),
        "teacher_up": gaussian(streams_of[7], (D, FF), D ** -0.5, 0.1875, ((0, 8), (1, 4))),
        "teacher_down": gaussian(streams_of[8], (D, FF), FF ** -0.5, 0.09375, ((0, 8), (1, 4))),
        "teacher_out": gaussian(streams_of[9], (PATCH, D), D ** -0.5, 0.1875),
        "student_patch": gaussian(streams_of[10], (PATCH, D), PATCH ** -0.5, 1.5),
        "student_mod": gaussian(streams_of[11], (D, 3, D), D ** -0.5, 0.1875, ((0, 8), (2, 4))),
        "student_up": gaussian(streams_of[12], (D, FF), D ** -0.5, 0.1875, ((0, 8), (1, 4))),
        "student_down": gaussian(streams_of[13], (D, FF), FF ** -0.5, 0.09375, ((0, 8), (1, 4))),
        "student_out": gaussian(streams_of[14], (PATCH, D), D ** -0.5, 0.1875),
    }


HALF_PI = 0.5 * math.pi
ROOT_TWO_PI = math.sqrt(2.0 / math.pi)

def plan(times):
    return (jnp.cos(HALF_PI * times), jnp.sin(HALF_PI * times))

def mixing(value):
    amount = jnp.int32(16)
    value = value ^ lax.shift_right_logical(value, amount)
    value = value * 73244475
    value = value ^ lax.shift_right_logical(value, amount)
    value = value * 73244475
    value = value ^ lax.shift_right_logical(value, amount)
    return value

def noise_of(seeds):
    total = SEQ * PATCH
    places = jnp.arange(total, dtype=jnp.int32).reshape(1, total // 128, 128)
    mixed = mixing(seeds[:, None, None] * 1103515245 + places * 40503 + 12345)
    uniform = (lax.shift_right_logical(mixed, jnp.int32(8)).astype(jnp.float32) + 0.5) * (1.0 / 16777216.0)
    return math.sqrt(2.0) * lax.erf_inv(2.0 * uniform - 1.0)

def time_features(times):
    half = D // 2
    freqs = jnp.exp(-math.log(10000.0) * jnp.arange(half, dtype=jnp.float32) / half)
    angle = (1000.0 * times)[:, None] * freqs[None, :]
    return jnp.concatenate([jnp.cos(angle), jnp.sin(angle)], axis=1)

def condition(times, labels, class_table):
    onehot = (labels[:, None] == jnp.arange(CLASSES, dtype=jnp.int32)[None, :]).astype(jnp.bfloat16)
    embedded = jnp.dot(onehot, class_table, preferred_element_type=jnp.float32)
    return jax.nn.silu(embedded + time_features(times)).astype(jnp.bfloat16)

def modulation(cond, weight):
    return jnp.einsum('nd,dkf->nkf', cond.astype(jnp.float32), weight.astype(jnp.float32), precision=lax.Precision.HIGHEST)

def positions():
    quarter = D // 4
    omega = 1.0 / 10000.0 ** (jnp.arange(quarter, dtype=jnp.float32) / quarter)
    side = math.isqrt(SEQ)
    cells = jnp.arange(SEQ, dtype=jnp.int32)
    grid_row = (cells // side).astype(jnp.float32)
    grid_col = (cells % side).astype(jnp.float32)
    row_angle = grid_row[:, None] * omega[None, :]
    col_angle = grid_col[:, None] * omega[None, :]
    return jnp.concatenate([jnp.sin(row_angle), jnp.cos(row_angle), jnp.sin(col_angle), jnp.cos(col_angle)], axis=1)

def layer_norm(values):
    center = values - lax.optimization_barrier(jnp.mean(values, axis=-1, keepdims=True))
    spread = lax.optimization_barrier(jnp.mean(center * center, axis=-1, keepdims=True))
    reciprocal = lax.rsqrt(spread + 1e-06)
    return (center * reciprocal, reciprocal)

def gelu_slope(pre):
    inner = ROOT_TWO_PI * (pre + 0.044715 * pre * pre * pre)
    tangent = jnp.tanh(inner)
    return 0.5 * (1.0 + tangent) + 0.5 * pre * (1.0 - tangent * tangent) * ROOT_TWO_PI * (1.0 + 3.0 * 0.044715 * pre * pre)

def contract_last(left, right):
    return lax.dot_general(left, right, (((1,), (1,)), ((), ())), preferred_element_type=jnp.float32)

def contract_first(left, right):
    return lax.dot_general(left, right, (((0,), (0,)), ((), ())), preferred_element_type=jnp.float32)

def network(state, mods, patch_weight, up_weight, down_weight, out_weight, pos):
    samples = state.shape[0]
    tokens = state.reshape(samples * SEQ, PATCH).astype(jnp.bfloat16)
    base = jnp.dot(tokens, patch_weight, preferred_element_type=jnp.float32).reshape(samples, SEQ, D) + pos[None]
    shift = mods[:, 0][:, None, :]
    scale = mods[:, 1][:, None, :]
    gate = mods[:, 2][:, None, :]
    normed, _ = layer_norm(base)
    act = (normed * (1.0 + scale) + shift).astype(jnp.bfloat16).reshape(samples * SEQ, D)
    pre = jnp.dot(act, up_weight, preferred_element_type=jnp.float32)
    hidden = jax.nn.gelu(pre, approximate=True).astype(jnp.bfloat16)
    width = FF // N_COL
    mixed = jnp.zeros((samples * SEQ, D), jnp.float32)
    for column in range(N_COL):
        part = contract_last(hidden[:, column * width:(column + 1) * width], down_weight[:, column * width:(column + 1) * width])
        rounded = lax.optimization_barrier(part.astype(jnp.bfloat16))
        mixed = mixed + rounded.astype(jnp.float32)
    later = base + gate * mixed.reshape(samples, SEQ, D)
    final, reciprocal = layer_norm(later)
    velocity = contract_last(final.astype(jnp.bfloat16).reshape(samples * SEQ, D), out_weight)
    return (velocity.reshape(samples, SEQ * PATCH // 128, 128), (act, pre, hidden, final, reciprocal, gate))

def reference(latents, labels, step_index, seeds, class_table, teacher_patch, teacher_mod, teacher_up, teacher_down, teacher_out, student_patch, student_mod, student_up, student_down, student_out):
    block = 8
    count = BATCH // block
    pos = positions()

    def one_block(carry, inputs):
        clean, names, steps, keys = inputs
        now = steps.astype(jnp.float32) / STEPS
        middle = now - 0.5 / STEPS
        ending = now - 1.0 / STEPS
        alpha, sigma = plan(now[:, None, None])
        alpha_mid, sigma_mid = plan(middle[:, None, None])
        alpha_end, sigma_end = plan(ending[:, None, None])
        cond_now = condition(now, names, class_table)
        cond_mid = condition(middle, names, class_table)
        teacher_now = modulation(cond_now, teacher_mod)
        teacher_mid = modulation(cond_mid, teacher_mod)
        student_mods = modulation(cond_now, student_mod)
        noisy = alpha * clean + sigma * noise_of(keys)
        first_v, _ = network(noisy, teacher_now, teacher_patch, teacher_up, teacher_down, teacher_out, pos)
        first_x = alpha * noisy - sigma * first_v
        halfway = alpha_mid * first_x + sigma_mid * (noisy - alpha * first_x) / sigma
        second_v, _ = network(halfway, teacher_mid, teacher_patch, teacher_up, teacher_down, teacher_out, pos)
        second_x = alpha_mid * halfway - sigma_mid * second_v
        landing = alpha_end * second_x + sigma_end * (halfway - alpha_mid * second_x) / sigma_mid
        ratio = sigma_end / sigma
        target = (landing - ratio * noisy) / (alpha_end - ratio * alpha)
        student_v, saved = network(noisy, student_mods, student_patch, student_up, student_down, student_out, pos)
        student_x = alpha * noisy - sigma * student_v
        weight = jnp.maximum(alpha * alpha / (sigma * sigma), 1.0)
        back_velocity = (-2.0 * sigma * weight * (student_x - target) / BATCH).reshape(block * SEQ, PATCH)
        act, pre, hidden, final, reciprocal, gate = saved
        back_final = jnp.dot(back_velocity, student_out.astype(jnp.float32), precision=lax.Precision.HIGHEST).reshape(block, SEQ, D)
        centre = lax.optimization_barrier(jnp.mean(back_final, axis=2, keepdims=True))
        along = lax.optimization_barrier(jnp.mean(back_final * final, axis=2, keepdims=True))
        back_mixed = (gate * (reciprocal * (back_final - centre - final * along))).astype(jnp.bfloat16).reshape(block * SEQ, D)
        down_term = contract_first(back_mixed, hidden)
        back_hidden = jnp.dot(back_mixed, student_down, preferred_element_type=jnp.float32)
        back_pre = (back_hidden * gelu_slope(pre)).astype(jnp.bfloat16)
        up_term = contract_first(act, back_pre)
        return ((carry[0] + up_term, carry[1] + down_term), None)
    inputs = (latents.reshape(count, block, SEQ * PATCH // 128, 128), labels.reshape(count, block), step_index.reshape(count, block), seeds.reshape(count, block))
    zeros = jnp.zeros((D, FF), jnp.float32)
    (up_gradient, down_gradient), _ = lax.scan(one_block, (zeros, zeros), inputs)
    return (up_gradient, down_gradient)
```

```python
import functools
import math

import jax
import jax.numpy as jnp
from jax import lax
from jax.experimental import pallas as pl
from jax.experimental.pallas import tpu as pltpu
from jax.sharding import PartitionSpec as P

D = 1152
CLASSES = 1000
SEQ = 256
PATCH = 16
STEPS = 8

HALF_PI = 0.5 * math.pi
ROOT_TWO_PI = math.sqrt(2.0 / math.pi)
PLANE = ("dp", "row")
F32 = jnp.float32
BF16 = jnp.bfloat16
VMEM_LIMIT = 60 * 1024 * 1024


def plan(times):
    return (jnp.cos(HALF_PI * times), jnp.sin(HALF_PI * times))


def mixing(value):
    amount = jnp.int32(16)
    value = value ^ lax.shift_right_logical(value, amount)
    value = value * 73244475
    value = value ^ lax.shift_right_logical(value, amount)
    value = value * 73244475
    value = value ^ lax.shift_right_logical(value, amount)
    return value


def noise_at(seeds, places):
    mixed = mixing(seeds * 1103515245 + places * 40503 + 12345)
    uniform = (lax.shift_right_logical(mixed, jnp.int32(8)).astype(F32) + 0.5) * (1.0 / 16777216.0)
    return math.sqrt(2.0) * lax.erf_inv(2.0 * uniform - 1.0)


def column_tile(width, most=384):
    best = 128
    for tile in range(128, most + 1, 128):
        if width % tile == 0:
            best = tile
    return best


def gelu(pre):
    inner = ROOT_TWO_PI * (pre + 0.044715 * (pre * pre * pre))
    return pre * (0.5 * (1.0 + jnp.tanh(inner)))


def gelu_slope(pre):
    inner = ROOT_TWO_PI * (pre + 0.044715 * pre * pre * pre)
    tangent = jnp.tanh(inner)
    return 0.5 * (1.0 + tangent) + 0.5 * pre * (1.0 - tangent * tangent) * ROOT_TWO_PI * (
        1.0 + 3.0 * 0.044715 * pre * pre
    )


def layer_norm(values):
    center = values - jnp.mean(values, axis=-1, keepdims=True)
    spread = jnp.mean(center * center, axis=-1, keepdims=True)
    reciprocal = lax.rsqrt(spread + 1e-06)
    return (center * reciprocal, reciprocal)


def dot(left, right, dims):
    return lax.dot_general(left, right, (dims, ((), ())), preferred_element_type=F32)


def upright(values):
    tokens = values.shape[1]
    eye = (
        lax.broadcasted_iota(jnp.int32, (tokens, tokens), 0)
        == lax.broadcasted_iota(jnp.int32, (tokens, tokens), 1)
    ).astype(F32).astype(BF16)
    return dot(eye, values.astype(BF16), ((1,), (1,))).astype(BF16)


def load_pieces(order, pieces, panel, sem):
    copies = []
    for spot, piece in enumerate(pieces):
        rows = piece.shape[0]
        start = pl.multiple_of(order[spot], 16) if len(pieces) > 1 else 0
        copies.append(pltpu.make_async_copy(piece, panel.at[pl.ds(start, rows), :], sem.at[spot]))
    for copy in copies:
        copy.start()
    return copies


def forward_kernel(pieces, first_mod, save, *refs):
    order, state, patch, pos, mods = refs[:5]
    refs = refs[5:]
    up_pieces, down_pieces, refs = refs[:pieces], refs[pieces : 2 * pieces], refs[2 * pieces :]
    groups, samples, _, tokens = state.shape
    outs, refs = refs[:groups], refs[groups:]
    if save:
        act, pre_out, hidden = refs[:3]
        refs = refs[3:]
        up, down, up_sem, down_sem = refs
    else:
        act, hidden, up, down, up_sem, down_sem = refs
    up_copies = load_pieces(order, up_pieces, up, up_sem)
    down_copies = load_pieces(order, down_pieces, down, down_sem)

    def embed(group, carry):
        for sample in range(samples):
            base = dot(upright(state[group, sample]), patch[...], ((1,), (0,))) + pos[group]
            normed, _ = layer_norm(base)
            shift = mods[sample, pl.ds(first_mod, 1), :]
            scale = mods[sample, pl.ds(first_mod + 1, 1), :]
            row = pl.multiple_of((group * samples + sample) * tokens, tokens)
            act[pl.ds(row, tokens), :] = (normed * (1.0 + scale) + shift).astype(BF16)
        return carry

    lax.fori_loop(0, groups, embed, 0)
    for copy in up_copies:
        copy.wait()
    width = up.shape[1]
    tile = column_tile(width)

    def first(step, carry):
        at = pl.multiple_of(step * tile, tile)
        pre = dot(act[...], up[:, pl.ds(at, tile)], ((1,), (0,)))
        if save:
            pre_out[:, pl.ds(at, tile)] = pre
        hidden[:, pl.ds(at, tile)] = gelu(pre).astype(BF16)
        return carry

    lax.fori_loop(0, width // tile, first, 0)
    for copy in down_copies:
        copy.wait()
    features = down.shape[0]
    feature_tile = column_tile(features)
    block = samples * tokens

    def second(step, carry):
        at = pl.multiple_of(step * feature_tile, feature_tile)
        part = dot(hidden[...], down[pl.ds(at, feature_tile), :], ((1,), (1,))).astype(BF16)
        for group in range(groups):
            outs[group][:, pl.ds(at, feature_tile)] = part[group * block : (group + 1) * block]
        return carry

    lax.fori_loop(0, features // feature_tile, second, 0)


def full(memory_space=pltpu.VMEM):
    return pl.BlockSpec(memory_space=memory_space)


def forward(order, state, patch, pos, mods, up_pieces, down_pieces, first_mod, save, name):
    groups, samples, _, tokens = state.shape
    count = len(up_pieces)
    total = groups * samples * tokens
    features = patch.shape[1]
    width = up_pieces[0].shape[1]
    out_shape = [jax.ShapeDtypeStruct((samples * tokens, features), BF16)] * groups
    scratch = [
        pltpu.VMEM((features, width), BF16),
        pltpu.VMEM((features, width), BF16),
        pltpu.SemaphoreType.DMA((count,)),
        pltpu.SemaphoreType.DMA((count,)),
    ]
    if save:
        out_shape = out_shape + [
            jax.ShapeDtypeStruct((total, features), BF16),
            jax.ShapeDtypeStruct((total, width), F32),
            jax.ShapeDtypeStruct((total, width), BF16),
        ]
    else:
        scratch = [pltpu.VMEM((total, features), BF16), pltpu.VMEM((total, width), BF16)] + scratch
    return pl.pallas_call(
        functools.partial(forward_kernel, count, first_mod, save),
        out_shape=out_shape,
        in_specs=[full(pltpu.SMEM)] + [full()] * 4 + [full(pl.ANY)] * (2 * count),
        out_specs=[full()] * len(out_shape),
        scratch_shapes=scratch,
        compiler_params=pltpu.CompilerParams(vmem_limit_bytes=VMEM_LIMIT),
        cost_estimate=pl.CostEstimate(
            flops=4 * total * features * width, bytes_accessed=8 * features * width, transcendentals=total * width
        ),
        name=name,
    )(order, state, patch, pos, mods, *up_pieces, *down_pieces)


def settle(parts, state, patch, pos, mods, out, gate_at, sample):
    tokens = state.shape[2]
    rows = slice(sample * tokens, (sample + 1) * tokens)
    mixed = parts[0][rows].astype(F32)
    for part in parts[1:]:
        mixed = mixed + part[rows].astype(F32)
    gate = mods[sample, gate_at : gate_at + 1, :]
    base = dot(upright(state[sample]), patch[...], ((1,), (0,))) + pos[...]
    final, reciprocal = layer_norm(base + gate * mixed)
    velocity = dot(out[...], final.astype(BF16), ((1,), (1,)))
    return velocity, final, reciprocal, gate


def middle_kernel(groups, *refs):
    coefs, state, patch, pos, mods, out = refs[:6]
    parts, halfway = refs[6 : 6 + groups], refs[6 + groups]
    for sample in range(state.shape[0]):
        velocity, _, _, _ = settle(parts, state, patch, pos, mods, out, 2, sample)
        noisy = state[sample]
        alpha, sigma = coefs[sample, 0], coefs[sample, 1]
        alpha_mid, sigma_mid = coefs[sample, 2], coefs[sample, 3]
        first_x = alpha * noisy - sigma * velocity
        halfway[sample] = alpha_mid * first_x + sigma_mid * (noisy - alpha * first_x) / sigma


def middle(coefs, state, patch, pos, mods, out, parts):
    groups = len(parts)
    return pl.pallas_call(
        functools.partial(middle_kernel, groups),
        out_shape=jax.ShapeDtypeStruct(state.shape, F32),
        in_specs=[full(pltpu.SMEM)] + [full()] * (5 + groups),
        out_specs=full(),
        compiler_params=pltpu.CompilerParams(vmem_limit_bytes=VMEM_LIMIT),
        cost_estimate=pl.CostEstimate(flops=10**9, bytes_accessed=2 * 10**6, transcendentals=0),
        name="middle",
    )(coefs, state, patch, pos, mods, out, *parts)


def last_kernel(groups, *refs):
    coefs, noisy_ref, half_ref, t_patch, s_patch, pos, mods, t_out, s_out = refs[:9]
    teacher, student, back = refs[9 : 9 + groups], refs[9 + groups : 9 + 2 * groups], refs[9 + 2 * groups]
    samples, _, tokens = noisy_ref.shape
    for sample in range(samples):
        second_v, _, _, _ = settle(teacher, half_ref, t_patch, pos, mods, t_out, 5, sample)
        student_v, final, reciprocal, gate = settle(
            student, noisy_ref, s_patch, pos, mods, s_out, 8, sample
        )
        noisy, halfway = noisy_ref[sample], half_ref[sample]
        alpha, sigma = coefs[sample, 0], coefs[sample, 1]
        alpha_mid, sigma_mid = coefs[sample, 2], coefs[sample, 3]
        alpha_end, sigma_end = coefs[sample, 4], coefs[sample, 5]
        ratio, gap, push = coefs[sample, 6], coefs[sample, 7], coefs[sample, 8]
        second_x = alpha_mid * halfway - sigma_mid * second_v
        landing = alpha_end * second_x + sigma_end * (halfway - alpha_mid * second_x) / sigma_mid
        target = (landing - ratio * noisy) / gap
        student_x = alpha * noisy - sigma * student_v
        back_velocity = push * (student_x - target)
        high = back_velocity.astype(BF16)
        rest = back_velocity - high.astype(F32)
        mid = rest.astype(BF16)
        low = (rest - mid.astype(F32)).astype(BF16)
        back_final = dot(upright(low), s_out[...], ((1,), (0,)))
        back_final = back_final + dot(upright(mid), s_out[...], ((1,), (0,)))
        back_final = back_final + dot(upright(high), s_out[...], ((1,), (0,)))
        centre = jnp.mean(back_final, axis=-1, keepdims=True)
        along = jnp.mean(back_final * final, axis=-1, keepdims=True)
        back[sample * tokens : (sample + 1) * tokens, :] = (
            gate * (reciprocal * (back_final - centre - final * along))
        ).astype(BF16)


def last(coefs, noisy, halfway, t_patch, s_patch, pos, mods, t_out, s_out, teacher, student):
    groups = len(teacher)
    samples, _, tokens = noisy.shape
    return pl.pallas_call(
        functools.partial(last_kernel, groups),
        out_shape=jax.ShapeDtypeStruct((samples * tokens, t_out.shape[1]), BF16),
        in_specs=[full(pltpu.SMEM)] + [full()] * (8 + 2 * groups),
        out_specs=full(),
        compiler_params=pltpu.CompilerParams(vmem_limit_bytes=VMEM_LIMIT),
        cost_estimate=pl.CostEstimate(flops=2 * 10**9, bytes_accessed=4 * 10**6, transcendentals=0),
        name="last",
    )(coefs, noisy, halfway, t_patch, s_patch, pos, mods, t_out, s_out, *teacher, *student)


def store_blocks(order, grad, blocks, sem):
    copies = []
    if len(blocks) == 1:
        copies.append(pltpu.make_async_copy(grad, blocks[0], sem.at[0]))
    else:
        mine, other = blocks
        count, rows = mine.shape[0], mine.shape[1]
        for spot in range(2 * count):
            start = pl.multiple_of(order[spot], 8)
            target = (mine, other)[spot % 2].at[spot // 2]
            copies.append(pltpu.make_async_copy(grad.at[pl.ds(start, rows), :], target, sem.at[spot]))
    for copy in copies:
        copy.start()
    for copy in copies:
        copy.wait()


def down_grad_kernel(groups, outs, *refs):
    order, refs = refs[0], refs[1:]
    backs, hidden, blocks = refs[:groups], refs[groups], refs[groups + 1 : groups + 1 + outs]
    back, grad, sem = refs[groups + 1 + outs :]
    rows = backs[0].shape[0]
    for group in range(groups):
        back[group * rows : (group + 1) * rows, :] = backs[group][...]
    features = back.shape[1]
    tile = column_tile(features)

    def step(index, carry):
        at = pl.multiple_of(index * tile, tile)
        grad[pl.ds(at, tile), :] = dot(back[:, pl.ds(at, tile)], hidden[...], ((0,), (0,)))
        return carry

    lax.fori_loop(0, features // tile, step, 0)
    store_blocks(order, grad, blocks, sem)


def up_grad_kernel(groups, pieces, outs, *refs):
    order, refs = refs[0], refs[1:]
    backs, act, pre = refs[:groups], refs[groups], refs[groups + 1]
    refs = refs[groups + 2 :]
    down_pieces, blocks, refs = refs[:pieces], refs[pieces : pieces + outs], refs[pieces + outs :]
    back, turned, down, grad, down_sem, sem = refs
    copies = load_pieces(order, down_pieces, down, down_sem)
    rows = backs[0].shape[0]
    for group in range(groups):
        back[group * rows : (group + 1) * rows, :] = backs[group][...]
    turned[...] = act[...].T
    for copy in copies:
        copy.wait()
    width = down.shape[1]
    tile = column_tile(width)

    def step(index, carry):
        at = pl.multiple_of(index * tile, tile)
        back_hidden = dot(back[...], down[:, pl.ds(at, tile)], ((1,), (0,)))
        back_pre = (back_hidden * gelu_slope(pre[:, pl.ds(at, tile)])).astype(BF16)
        grad[:, pl.ds(at, tile)] = dot(turned[...], back_pre, ((1,), (0,)))
        return carry

    lax.fori_loop(0, width // tile, step, 0)
    store_blocks(order, grad, blocks, sem)


def block_shapes(count, features, width):
    if count == 1:
        return [jax.ShapeDtypeStruct((features, width), F32)]
    return [jax.ShapeDtypeStruct((count // 2, features // count, width), F32)] * 2


def down_grad(order, backs, hidden, count):
    features = backs[0].shape[1]
    total, width = hidden.shape
    shapes = block_shapes(count, features, width)
    return pl.pallas_call(
        functools.partial(down_grad_kernel, len(backs), len(shapes)),
        out_shape=shapes,
        in_specs=[full(pltpu.SMEM)] + [full()] * (len(backs) + 1),
        out_specs=[full(pl.ANY)] * len(shapes),
        scratch_shapes=[
            pltpu.VMEM((total, features), BF16),
            pltpu.VMEM((features, width), F32),
            pltpu.SemaphoreType.DMA((count,)),
        ],
        compiler_params=pltpu.CompilerParams(vmem_limit_bytes=VMEM_LIMIT),
        cost_estimate=pl.CostEstimate(
            flops=2 * total * features * width, bytes_accessed=8 * features * width, transcendentals=0
        ),
        name="down_grad",
    )(order, *backs, hidden)


def up_grad(order, backs, act, pre, down_pieces, count):
    features = backs[0].shape[1]
    total, width = pre.shape
    shapes = block_shapes(count, features, width)
    pieces = len(down_pieces)
    return pl.pallas_call(
        functools.partial(up_grad_kernel, len(backs), pieces, len(shapes)),
        out_shape=shapes,
        in_specs=[full(pltpu.SMEM)] + [full()] * (len(backs) + 2) + [full(pl.ANY)] * pieces,
        out_specs=[full(pl.ANY)] * len(shapes),
        scratch_shapes=[
            pltpu.VMEM((total, features), BF16),
            pltpu.VMEM((features, total), BF16),
            pltpu.VMEM((features, width), BF16),
            pltpu.VMEM((features, width), F32),
            pltpu.SemaphoreType.DMA((pieces,)),
            pltpu.SemaphoreType.DMA((count,)),
        ],
        compiler_params=pltpu.CompilerParams(vmem_limit_bytes=VMEM_LIMIT),
        cost_estimate=pl.CostEstimate(
            flops=4 * total * features * width, bytes_accessed=8 * features * width, transcendentals=total * width
        ),
        name="up_grad",
    )(order, *backs, act, pre, *down_pieces)


def swap_plane(value, flip, size):
    return lax.ppermute(value, PLANE, [(spot, spot ^ flip) for spot in range(size)])


def swap_col(value, flip, size):
    return lax.ppermute(value, "col", [(spot, spot ^ flip) for spot in range(size)])


def spread_plane(shard, size):
    pieces = {0: shard}
    for flip in range(2, size, 2):
        pieces[flip] = swap_plane(shard, flip, size)
    for flip in range(0, size, 2):
        pieces[flip ^ 1] = swap_plane(pieces[flip], 1, size)
    return [pieces[flip] for flip in range(size)]


def spread_col(value, size):
    return [value] + [swap_col(value, flip, size) for flip in range(1, size)]


def condition(times, embedded, offset, rows):
    half = D // 2
    places = offset + jnp.arange(rows, dtype=jnp.int32)
    low = places < half
    power = jnp.where(low, places, places - half).astype(F32)
    freqs = jnp.exp(-math.log(10000.0) * power / half)
    angle = (1000.0 * times)[:, None] * freqs[None, :]
    features = jnp.where(low[None, :], jnp.cos(angle), jnp.sin(angle))
    return jax.nn.silu(embedded + features).astype(BF16)


def modulations(labels, step_index, class_table, teacher_mod, student_mod, fast, plane, columns, col):
    samples = labels.shape[0]
    rows = teacher_mod.shape[0]
    packed = labels * 16 + step_index
    if fast:
        everyone = jnp.concatenate(spread_plane(packed, plane), axis=0)
    else:
        everyone = lax.all_gather(packed, PLANE, axis=0, tiled=True)
    all_labels, all_steps = everyone // 16, everyone % 16
    all_now = all_steps.astype(F32) / STEPS
    offset = lax.axis_index(PLANE) * rows
    table = lax.dynamic_slice_in_dim(class_table, offset, rows, 1)
    onehot = (all_labels[:, None] == jnp.arange(CLASSES, dtype=jnp.int32)[None, :]).astype(BF16)
    embedded = jnp.dot(onehot, table, preferred_element_type=F32)
    rows_now = condition(all_now, embedded, offset, rows)
    rows_mid = condition(all_now - 0.5 / STEPS, embedded, offset, rows)
    count = rows_now.shape[0]
    share = teacher_mod.shape[2]
    teacher_flat = teacher_mod.reshape(rows, 3 * share)
    student_flat = student_mod.reshape(rows, 3 * share)
    teacher_part = jnp.dot(
        jnp.concatenate([rows_now, rows_mid], axis=0), teacher_flat, preferred_element_type=F32
    )
    student_part = jnp.dot(rows_now, student_flat, preferred_element_type=F32)
    part = jnp.stack([teacher_part[:count], teacher_part[count:], student_part], axis=1)
    if fast:
        part = part.reshape(plane // 2, 2, samples, 3, 3 * share)
        pair = part[:, 0] + swap_plane(part[:, 1], 1, plane)
        own = pair[0]
        for flip in range(1, plane // 2):
            own = own + swap_plane(pair[flip], 2 * flip, plane)
    else:
        own = lax.psum_scatter(part, PLANE, scatter_dimension=0, tiled=True)
    own = own.reshape(samples, 9, share)
    gathered = jnp.stack(spread_col(own, columns), axis=0)
    ordered = jnp.take(gathered, jnp.arange(columns) ^ col, axis=0)
    return jnp.moveaxis(ordered, 0, 2).reshape(samples, 9, columns * share)


def positions(chunks, tokens):
    quarter = D // 4
    omega = 1.0 / 10000.0 ** (jnp.arange(quarter, dtype=F32) / quarter)
    side = math.isqrt(SEQ)
    angle = jnp.arange(side, dtype=F32)[:, None] * omega[None, :]
    angle = lax.optimization_barrier(angle)
    table = jnp.concatenate([jnp.sin(angle), jnp.cos(angle)], axis=1)
    down = jnp.broadcast_to(table[:, None, :], (side, side, D // 2))
    across = jnp.broadcast_to(table[None, :, :], (side, side, D // 2))
    whole = jnp.concatenate([down, across], axis=2).reshape(SEQ // tokens, tokens, D)
    return jnp.take(whole, chunks, axis=0)


def body(
    latents,
    labels,
    step_index,
    seeds,
    class_table,
    teacher_patch,
    teacher_mod,
    teacher_up,
    teacher_down,
    teacher_out,
    student_patch,
    student_mod,
    student_up,
    student_down,
    student_out,
):
    samples = latents.shape[0]
    plane = lax.axis_size(PLANE)
    columns = lax.axis_size("col")
    batch_total = samples * plane
    col = lax.axis_index("col")
    spot = lax.axis_index(PLANE)
    rows = teacher_up.shape[0]
    tokens = SEQ // columns
    fast = rows % 16 == 0 and plane <= 8
    count = plane if fast else 1

    def gather(shard):
        if fast:
            return spread_plane(shard, plane)
        return [lax.all_gather(shard, PLANE, axis=0, tiled=True)]

    order = ((jnp.arange(count, dtype=jnp.int32) ^ spot) * rows).astype(jnp.int32)
    teacher_up_pieces = gather(teacher_up)
    mods = modulations(
        labels, step_index, class_table, teacher_mod, student_mod, fast, plane, columns, col
    )
    teacher_down_pieces = gather(teacher_down)
    student_up_pieces = gather(student_up)
    student_down_pieces = gather(student_down)

    chunks = jnp.arange(columns, dtype=jnp.int32) ^ col
    pos = positions(chunks, tokens)
    now = step_index.astype(F32) / STEPS
    alpha, sigma = plan(now)
    alpha_mid, sigma_mid = plan(now - 0.5 / STEPS)
    alpha_end, sigma_end = plan(now - 1.0 / STEPS)
    ratio = sigma_end / sigma
    weight = jnp.maximum(alpha * alpha / (sigma * sigma), 1.0)
    push = -2.0 * sigma * weight / batch_total
    coefs = jnp.stack(
        [alpha, sigma, alpha_mid, sigma_mid, alpha_end, sigma_end, ratio, alpha_end - ratio * alpha, push],
        axis=1,
    )
    clean = latents.reshape(samples, columns, tokens, PATCH)
    clean = jnp.take(jnp.transpose(clean, (1, 0, 3, 2)), chunks, axis=0)
    token = chunks[:, None, None, None] * tokens + jnp.arange(tokens, dtype=jnp.int32)
    places = token * PATCH + jnp.arange(PATCH, dtype=jnp.int32)[None, None, :, None]
    shaped = (1, samples, 1, 1)
    noisy = alpha.reshape(shaped) * clean + sigma.reshape(shaped) * noise_at(
        seeds.reshape(shaped), places
    )

    def share(parts):
        return [parts[0]] + [swap_col(parts[flip], flip, columns) for flip in range(1, columns)]

    teacher_args = (teacher_patch, pos, mods, teacher_up_pieces, teacher_down_pieces)
    first = share(forward(order, noisy, *teacher_args, 0, False, "teacher_now"))
    halfway = middle(coefs, noisy[0], teacher_patch, pos[0], mods, teacher_out, first)
    half_all = jnp.stack(spread_col(halfway, columns), axis=0)
    second = share(forward(order, half_all, *teacher_args, 3, False, "teacher_mid"))
    saved = forward(
        order, noisy, student_patch, pos, mods, student_up_pieces, student_down_pieces, 6, True, "student"
    )
    student = share(saved[:columns])
    act, pre, hidden = saved[columns:]
    back = last(
        coefs,
        noisy[0],
        halfway,
        teacher_patch,
        student_patch,
        pos[0],
        mods,
        teacher_out,
        student_out,
        second,
        student,
    )
    backs = spread_col(back, columns)

    def reduce_gradient(blocks):
        if not fast:
            return lax.psum_scatter(blocks[0], PLANE, scatter_dimension=0, tiled=True)
        mine, other = blocks
        pair = mine + swap_plane(other, 1, plane)
        total = pair[0]
        for flip in range(1, plane // 2):
            total = total + swap_plane(pair[flip].astype(BF16), 2 * flip, plane).astype(F32)
        return total

    down_gradient = reduce_gradient(down_grad(order, backs, hidden, count))
    up_gradient = reduce_gradient(up_grad(order, backs, act, pre, student_down_pieces, count))
    return (up_gradient, down_gradient)


def solution(mesh):
    rows = P(("dp", "row"), "col")
    mod = P(("dp", "row"), None, "col")
    batch = P(("dp", "row"))
    placed = (
        P(("dp", "row"), None, None),
        batch,
        batch,
        batch,
        P(),
        P(),
        mod,
        rows,
        rows,
        P(),
        P(),
        mod,
        rows,
        rows,
        P(),
    )
    return jax.shard_map(
        body, mesh=mesh, in_specs=placed, out_specs=(rows, rows), check_vma=False
    )
```

```python
import functools
import math

import jax
import jax.numpy as jnp
from jax import lax
from jax.experimental import pallas as pl
from jax.experimental.pallas import tpu as pltpu
from jax.sharding import PartitionSpec as P


D = 1152
CLASSES = 1000
SEQ = 256
PATCH = 16
STEPS = 8

HALF_PI = 0.5 * math.pi
ROOT_TWO_PI = math.sqrt(2.0 / math.pi)
PLANE = ("dp", "row")
F32 = jnp.float32
BF16 = jnp.bfloat16
VMEM_LIMIT = 30 * 1024 * 1024


def plan(times):
    return (jnp.cos(HALF_PI * times), jnp.sin(HALF_PI * times))


def mixing(value):
    amount = jnp.int32(16)
    value = value ^ lax.shift_right_logical(value, amount)
    value = value * 73244475
    value = value ^ lax.shift_right_logical(value, amount)
    value = value * 73244475
    value = value ^ lax.shift_right_logical(value, amount)
    return value


def noise_at(seeds, places):
    mixed = mixing(seeds * 1103515245 + places * 40503 + 12345)
    uniform = (lax.shift_right_logical(mixed, jnp.int32(8)).astype(F32) + 0.5) * (1.0 / 16777216.0)
    return math.sqrt(2.0) * lax.erf_inv(2.0 * uniform - 1.0)


def column_tile(width, most=1152):
    best = 128
    for tile in range(128, most + 1, 128):
        if width % tile == 0:
            best = tile
    return best


def gelu(pre):
    inner = ROOT_TWO_PI * (pre + 0.044715 * (pre * pre * pre))
    return pre * (0.5 * (1.0 + jnp.tanh(inner)))


def gelu_slope(pre):
    inner = ROOT_TWO_PI * (pre + 0.044715 * pre * pre * pre)
    tangent = jnp.tanh(inner)
    return 0.5 * (1.0 + tangent) + 0.5 * pre * (1.0 - tangent * tangent) * ROOT_TWO_PI * (
        1.0 + 3.0 * 0.044715 * pre * pre
    )


def layer_norm(values):
    center = values - jnp.mean(values, axis=-1, keepdims=True)
    spread = jnp.mean(center * center, axis=-1, keepdims=True)
    reciprocal = lax.rsqrt(spread + 1e-06)
    return (center * reciprocal, reciprocal)


def dot(left, right, dims):
    return lax.dot_general(left, right, (dims, ((), ())), preferred_element_type=F32)


def upright(values):
    tokens = values.shape[1]
    eye = (
        lax.broadcasted_iota(jnp.int32, (tokens, tokens), 0)
        == lax.broadcasted_iota(jnp.int32, (tokens, tokens), 1)
    ).astype(F32).astype(BF16)
    return dot(eye, values.astype(BF16), ((1,), (1,))).astype(BF16)


def place(base, down, across):
    side = across.shape[0]
    parts = []
    for row in range(base.shape[0] // side):
        parts.append(base[row * side : (row + 1) * side] + (down[row : row + 1] + across))
    return jnp.concatenate(parts, axis=0)


def load_pieces(order, pieces, panel, sem):
    copies = []
    for spot, piece in enumerate(pieces):
        rows = piece.shape[0]
        start = pl.multiple_of(order[spot], 16) if len(pieces) > 1 else 0
        copies.append(pltpu.make_async_copy(piece, panel.at[pl.ds(start, rows), :], sem.at[spot]))
    for copy in copies:
        copy.start()
    return copies


def forward_kernel(pieces, first_mod, save, per_set, *refs):
    order, state, patch, down_pos, across, mods = refs[:6]
    refs = refs[6:]
    up_pieces, down_pieces, refs = refs[:pieces], refs[pieces : 2 * pieces], refs[2 * pieces :]
    groups, samples, _, tokens = state.shape
    outs, refs = refs[:groups], refs[groups:]
    if save:
        act, pre_out, hidden = refs[:3]
        refs = refs[3:]
        up, down, up_sem, down_sem = refs
    else:
        act, hidden, up, down, up_sem, down_sem = refs
    up_copies = load_pieces(order, up_pieces, up, up_sem)
    down_copies = load_pieces(order, down_pieces, down, down_sem)

    def embed(group, carry):
        for sample in range(samples):
            base = dot(upright(state[group, sample]), patch[...], ((1,), (0,)))
            base = place(base, down_pos[group], across[...])
            normed, _ = layer_norm(base)
            spot = (group // per_set) * samples + sample if per_set else sample
            shift = mods[spot, pl.ds(first_mod, 1), :]
            scale = mods[spot, pl.ds(first_mod + 1, 1), :]
            row = pl.multiple_of((group * samples + sample) * tokens, tokens)
            act[pl.ds(row, tokens), :] = (normed * (1.0 + scale) + shift).astype(BF16)
        return carry

    lax.fori_loop(0, groups, embed, 0)
    for copy in up_copies:
        copy.wait()
    block = samples * tokens
    halves = 2 if groups % 2 == 0 else 1
    tall = groups // halves * block

    def first(step, carry):
        at = pl.multiple_of(step * tall, tall)
        pre = dot(act[pl.ds(at, tall), :], up[...], ((1,), (0,)))
        if save:
            pre_out[pl.ds(at, tall), :] = pre
        hidden[pl.ds(at, tall), :] = gelu(pre).astype(BF16)
        return carry

    lax.fori_loop(0, halves, first, 0)
    for copy in down_copies:
        copy.wait()
    part = dot(hidden[...], down[...], ((1,), (1,))).astype(BF16)
    for group in range(groups):
        outs[group][...] = part[group * block : (group + 1) * block]


def full(memory_space=pltpu.VMEM):
    return pl.BlockSpec(memory_space=memory_space)


def forward(order, state, patch, pos, mods, up_pieces, down_pieces, first_mod, save, per_set=0):
    groups, samples, _, tokens = state.shape
    count = len(up_pieces)
    total = groups * samples * tokens
    features = patch.shape[1]
    width = up_pieces[0].shape[1]
    out_shape = [jax.ShapeDtypeStruct((samples * tokens, features), BF16)] * groups
    scratch = [
        pltpu.VMEM((features, width), BF16),
        pltpu.VMEM((features, width), BF16),
        pltpu.SemaphoreType.DMA((count,)),
        pltpu.SemaphoreType.DMA((count,)),
    ]
    if save:
        out_shape = out_shape + [
            jax.ShapeDtypeStruct((total, features), BF16),
            jax.ShapeDtypeStruct((total, width), F32),
            jax.ShapeDtypeStruct((total, width), BF16),
        ]
    else:
        scratch = [pltpu.VMEM((total, features), BF16), pltpu.VMEM((total, width), BF16)] + scratch
    return pl.pallas_call(
        functools.partial(forward_kernel, count, first_mod, save, per_set),
        out_shape=out_shape,
        in_specs=[full(pltpu.SMEM)] + [full()] * 5 + [full(pltpu.HBM)] * (2 * count),
        out_specs=[full()] * len(out_shape),
        scratch_shapes=scratch,
        compiler_params=pltpu.CompilerParams(vmem_limit_bytes=VMEM_LIMIT),
        cost_estimate=pl.CostEstimate(
            flops=4 * total * features * width, bytes_accessed=8 * features * width, transcendentals=total * width
        ),
    )(order, state, patch, *pos, mods, *up_pieces, *down_pieces)


def settle(parts, state, patch, down_pos, across, mods, out, gate_at, sample):
    tokens = state.shape[2]
    rows = slice(sample * tokens, (sample + 1) * tokens)
    mixed = parts[0][rows].astype(F32)
    for part in parts[1:]:
        mixed = mixed + part[rows].astype(F32)
    gate = mods[sample, gate_at : gate_at + 1, :]
    base = dot(upright(state[sample]), patch[...], ((1,), (0,)))
    base = place(base, down_pos[0], across[...])
    final, reciprocal = layer_norm(base + gate * mixed)
    velocity = dot(out[...], final.astype(BF16), ((1,), (1,)))
    return velocity, final, reciprocal, gate


def middle_kernel(groups, *refs):
    coefs, state, patch, down_pos, across, mods, out = refs[:7]
    parts, halfway = refs[7 : 7 + groups], refs[7 + groups]
    for sample in range(state.shape[0]):
        velocity, _, _, _ = settle(parts, state, patch, down_pos, across, mods, out, 2, sample)
        noisy = state[sample]
        alpha, sigma = coefs[sample, 0], coefs[sample, 1]
        alpha_mid, sigma_mid = coefs[sample, 2], coefs[sample, 3]
        first_x = alpha * noisy - sigma * velocity
        halfway[sample] = alpha_mid * first_x + sigma_mid * (noisy - alpha * first_x) / sigma


def middle(coefs, state, patch, pos, mods, out, parts):
    groups = len(parts)
    return pl.pallas_call(
        functools.partial(middle_kernel, groups),
        out_shape=jax.ShapeDtypeStruct(state.shape, F32),
        in_specs=[full(pltpu.SMEM)] + [full()] * (6 + groups),
        out_specs=full(),
        compiler_params=pltpu.CompilerParams(vmem_limit_bytes=VMEM_LIMIT),
        cost_estimate=pl.CostEstimate(flops=10**9, bytes_accessed=2 * 10**6, transcendentals=0),
        name="middle",
    )(coefs, state, patch, *pos, mods, out, *parts)


def last_kernel(groups, *refs):
    coefs, noisy_ref, half_ref, t_patch, s_patch, down_pos, across, mods, t_out, s_out = refs[:10]
    refs = refs[10:]
    teacher, student, back = refs[:groups], refs[groups : 2 * groups], refs[2 * groups]
    samples, _, tokens = noisy_ref.shape
    for sample in range(samples):
        second_v, _, _, _ = settle(
            teacher, half_ref, t_patch, down_pos, across, mods, t_out, 5, sample
        )
        student_v, final, reciprocal, gate = settle(
            student, noisy_ref, s_patch, down_pos, across, mods, s_out, 8, sample
        )
        noisy, halfway = noisy_ref[sample], half_ref[sample]
        alpha, sigma = coefs[sample, 0], coefs[sample, 1]
        alpha_mid, sigma_mid = coefs[sample, 2], coefs[sample, 3]
        alpha_end, sigma_end = coefs[sample, 4], coefs[sample, 5]
        ratio, gap, push = coefs[sample, 6], coefs[sample, 7], coefs[sample, 8]
        second_x = alpha_mid * halfway - sigma_mid * second_v
        landing = alpha_end * second_x + sigma_end * (halfway - alpha_mid * second_x) / sigma_mid
        target = (landing - ratio * noisy) / gap
        student_x = alpha * noisy - sigma * student_v
        back_velocity = push * (student_x - target)
        high = back_velocity.astype(BF16)
        rest = back_velocity - high.astype(F32)
        mid = rest.astype(BF16)
        low = (rest - mid.astype(F32)).astype(BF16)
        back_final = dot(upright(low), s_out[...], ((1,), (0,)))
        back_final = back_final + dot(upright(mid), s_out[...], ((1,), (0,)))
        back_final = back_final + dot(upright(high), s_out[...], ((1,), (0,)))
        centre = jnp.mean(back_final, axis=-1, keepdims=True)
        along = jnp.mean(back_final * final, axis=-1, keepdims=True)
        back[sample * tokens : (sample + 1) * tokens, :] = (
            gate * (reciprocal * (back_final - centre - final * along))
        ).astype(BF16)


def last(coefs, noisy, halfway, t_patch, s_patch, pos, mods, t_out, s_out, teacher, student):
    groups = len(teacher)
    samples, _, tokens = noisy.shape
    return pl.pallas_call(
        functools.partial(last_kernel, groups),
        out_shape=jax.ShapeDtypeStruct((samples * tokens, t_out.shape[1]), BF16),
        in_specs=[full(pltpu.SMEM)] + [full()] * (9 + 2 * groups),
        out_specs=full(),
        compiler_params=pltpu.CompilerParams(vmem_limit_bytes=VMEM_LIMIT),
        cost_estimate=pl.CostEstimate(flops=2 * 10**9, bytes_accessed=4 * 10**6, transcendentals=0),
        name="last",
    )(coefs, noisy, halfway, t_patch, s_patch, *pos, mods, t_out, s_out, *teacher, *student)


def store_blocks(order, grad, blocks, sem):
    copies = []
    if len(blocks) == 1:
        copies.append(pltpu.make_async_copy(grad, blocks[0], sem.at[0]))
    else:
        mine, other = blocks
        count, rows = mine.shape[0], mine.shape[1]
        for spot in range(2 * count):
            start = pl.multiple_of(order[spot], 8)
            target = (mine, other)[spot % 2].at[spot // 2]
            copies.append(pltpu.make_async_copy(grad.at[pl.ds(start, rows), :], target, sem.at[spot]))
    for copy in copies:
        copy.start()
    for copy in copies:
        copy.wait()


def weight_grad_kernel(groups, outs, *refs):
    order, refs = refs[0], refs[1:]
    backs, hidden, blocks = refs[:groups], refs[groups], refs[groups + 1 : groups + 1 + outs]
    back, grad, sem = refs[groups + 1 + outs :]
    rows = backs[0].shape[0]
    for group in range(groups):
        back[group * rows : (group + 1) * rows, :] = backs[group][...]
    features = back.shape[1]
    tile = column_tile(features)

    def step(index, carry):
        at = pl.multiple_of(index * tile, tile)
        grad[pl.ds(at, tile), :] = dot(back[:, pl.ds(at, tile)], hidden[...], ((0,), (0,)))
        return carry

    lax.fori_loop(0, features // tile, step, 0)
    store_blocks(order, grad, blocks, sem)


def back_pre_kernel(groups, pieces, *refs):
    order, refs = refs[0], refs[1:]
    backs, pre, refs = refs[:groups], refs[groups], refs[groups + 1 :]
    down_pieces, back_pre, back, down, sem = refs[:pieces], *refs[pieces:]
    copies = load_pieces(order, down_pieces, down, sem)
    rows = backs[0].shape[0]
    for group in range(groups):
        back[group * rows : (group + 1) * rows, :] = backs[group][...]
    for copy in copies:
        copy.wait()
    back_hidden = dot(back[...], down[...], ((1,), (0,)))
    back_pre[...] = (back_hidden * gelu_slope(pre[...])).astype(BF16)


def block_shapes(count, features, width):
    if count == 1:
        return [jax.ShapeDtypeStruct((features, width), F32)]
    return [jax.ShapeDtypeStruct((count // 2, features // count, width), F32)] * 2


def weight_grad(order, backs, hidden, count):
    features = backs[0].shape[1]
    total, width = hidden.shape
    shapes = block_shapes(count, features, width)
    return pl.pallas_call(
        functools.partial(weight_grad_kernel, len(backs), len(shapes)),
        out_shape=shapes,
        in_specs=[full(pltpu.SMEM)] + [full()] * (len(backs) + 1),
        out_specs=[full(pltpu.HBM)] * len(shapes),
        scratch_shapes=[
            pltpu.VMEM((total, features), BF16),
            pltpu.VMEM((features, width), F32),
            pltpu.SemaphoreType.DMA((count,)),
        ],
        compiler_params=pltpu.CompilerParams(vmem_limit_bytes=VMEM_LIMIT),
        cost_estimate=pl.CostEstimate(
            flops=2 * total * features * width, bytes_accessed=8 * features * width, transcendentals=0
        ),
    )(order, *backs, hidden)


def back_through(order, backs, pre, down_pieces):
    features = backs[0].shape[1]
    total, width = pre.shape
    pieces = len(down_pieces)
    return pl.pallas_call(
        functools.partial(back_pre_kernel, len(backs), pieces),
        out_shape=jax.ShapeDtypeStruct((total, width), BF16),
        in_specs=[full(pltpu.SMEM)] + [full()] * (len(backs) + 1) + [full(pltpu.HBM)] * pieces,
        out_specs=full(),
        scratch_shapes=[
            pltpu.VMEM((total, features), BF16),
            pltpu.VMEM((features, width), BF16),
            pltpu.SemaphoreType.DMA((pieces,)),
        ],
        compiler_params=pltpu.CompilerParams(vmem_limit_bytes=VMEM_LIMIT),
        cost_estimate=pl.CostEstimate(
            flops=2 * total * features * width, bytes_accessed=8 * features * width, transcendentals=total * width
        ),
        name="back_pre",
    )(order, *backs, pre, *down_pieces)


def after(value, earlier):
    return lax.optimization_barrier((value, earlier))[0]


def swap_plane(value, flip, size):
    return lax.ppermute(value, PLANE, [(spot, spot ^ flip) for spot in range(size)])


def swap_col(value, flip, size):
    return lax.ppermute(value, "col", [(spot, spot ^ flip) for spot in range(size)])


def swap_both(value, flip, plane, columns):
    pairs = []
    for spot in range(plane):
        for col in range(columns):
            pairs.append((spot * columns + col, (spot ^ flip[0]) * columns + (col ^ flip[1])))
    return lax.ppermute(value, ("dp", "row", "col"), pairs)


def chips_of_plane(even, odd, size):
    return [even] + [swap_plane((even, odd)[flip % 2], 2 * flip, size) for flip in range(1, size // 2)]


def both_cores(shards, size):
    pieces = []
    for shard in shards:
        pieces += [shard, swap_plane(shard, 1, size)]
    return pieces


def spread_col(value, size):
    return [value] + [swap_col(value, flip, size) for flip in range(1, size)]


def condition(times, embedded, offset, rows):
    half = D // 2
    places = offset + jnp.arange(rows, dtype=jnp.int32)
    low = places < half
    power = jnp.where(low, places, places - half).astype(F32)
    freqs = jnp.exp(-math.log(10000.0) * power / half)
    angle = (1000.0 * times)[:, None] * freqs[None, :]
    features = jnp.where(low[None, :], jnp.cos(angle), jnp.sin(angle))
    return jax.nn.silu(embedded + features).astype(BF16)


def modulation_part(labels, step_index, class_table, teacher_mod, student_mod, earlier, fast, plane):
    rows = teacher_mod.shape[0]
    packed = labels * 16 + step_index
    if fast:
        others = [swap_plane(packed, flip, plane) for flip in range(1, plane)]
        everyone = jnp.concatenate([packed] + others, axis=0)
    else:
        everyone = lax.all_gather(packed, PLANE, axis=0, tiled=True)
    everyone = after(everyone, earlier)
    all_labels, all_steps = everyone // 16, everyone % 16
    all_now = all_steps.astype(F32) / STEPS
    offset = lax.axis_index(PLANE) * rows
    table = lax.dynamic_slice_in_dim(class_table, offset, rows, 1)
    onehot = (all_labels[:, None] == jnp.arange(CLASSES, dtype=jnp.int32)[None, :]).astype(BF16)
    embedded = jnp.dot(onehot, table, preferred_element_type=F32)
    rows_now = condition(all_now, embedded, offset, rows)
    rows_mid = condition(all_now - 0.5 / STEPS, embedded, offset, rows)
    count = rows_now.shape[0]
    share = teacher_mod.shape[2]
    teacher_flat = teacher_mod.reshape(rows, 3 * share)
    student_flat = student_mod.reshape(rows, 3 * share)
    teacher_part = jnp.dot(
        jnp.concatenate([rows_now, rows_mid], axis=0), teacher_flat, preferred_element_type=F32
    )
    student_part = jnp.dot(rows_now, student_flat, preferred_element_type=F32)
    return jnp.concatenate([teacher_part[:count], teacher_part[count:], student_part], axis=1)


def modulation_sum(part, samples, fast, square, plane):
    if not fast:
        return lax.psum_scatter(part, PLANE, scatter_dimension=0, tiled=True)[None]
    part = part.reshape(plane // 2, 2, samples, part.shape[1])
    pair = part[:, 0] + swap_plane(part[:, 1], 1, plane)
    sets = 2 if square else 1
    own = jnp.stack([pair[other] for other in range(sets)], axis=0)
    for flip in range(1, plane // 2):
        sent = jnp.stack([pair[flip ^ other] for other in range(sets)], axis=0)
        own = own + swap_plane(sent, 2 * flip, plane)
    return own


def modulation_columns(own, columns, col):
    sets, samples = own.shape[:2]
    own = own.reshape(sets * samples, 9, own.shape[2] // 9)
    gathered = spread_col(own, columns)
    ordered = []
    for place_at in range(columns):
        piece = gathered[place_at]
        for other in range(1, columns):
            piece = jnp.where(col == other, gathered[place_at ^ other], piece)
        ordered.append(piece)
    return jnp.concatenate(ordered, axis=2)


def positions(chunks, tokens):
    quarter = D // 4
    omega = 1.0 / 10000.0 ** (jnp.arange(quarter, dtype=F32) / quarter)
    side = math.isqrt(SEQ)
    span = tokens // side
    angle = jnp.arange(side, dtype=F32)[:, None] * omega[None, :]
    across = jnp.concatenate([jnp.zeros((side, D // 2), F32), jnp.sin(angle), jnp.cos(angle)], axis=1)
    grid_rows = chunks[:, None] * span + jnp.arange(span, dtype=jnp.int32)
    turn = grid_rows.astype(F32)[:, :, None] * omega
    down = jnp.concatenate(
        [jnp.sin(turn), jnp.cos(turn), jnp.zeros((chunks.shape[0], span, D // 2), F32)], axis=2
    )
    return down, across


def body(
    latents,
    labels,
    step_index,
    seeds,
    class_table,
    teacher_patch,
    teacher_mod,
    teacher_up,
    teacher_down,
    teacher_out,
    student_patch,
    student_mod,
    student_up,
    student_down,
    student_out,
):
    samples = latents.shape[0]
    plane = lax.axis_size(PLANE)
    columns = lax.axis_size("col")
    batch_total = samples * plane
    col = lax.axis_index("col")
    spot = lax.axis_index(PLANE)
    rows = teacher_up.shape[0]
    tokens = SEQ // columns
    fast = rows % 16 == 0 and plane <= 8
    count = plane if fast else 1

    order = ((jnp.arange(count, dtype=jnp.int32) ^ spot) * rows).astype(jnp.int32)

    square = fast and columns == 4 and plane >= 4
    odd_chip = (spot // 2) % 2 == 1

    def chips(even, odd=None):
        if fast:
            return chips_of_plane(even, even if odd is None else odd, plane)
        return [lax.all_gather(even, PLANE, axis=0, tiled=True)]

    def cores(shards):
        return both_cores(shards, plane) if fast else shards

    def teacher_shards(shard, abroad):
        if not square:
            return (shard,)
        return jnp.where(odd_chip, abroad, shard), jnp.where(odd_chip, shard, abroad)

    up_abroad = swap_col(teacher_up, 2, columns) if square else teacher_up
    down_abroad = swap_col(after(teacher_down, up_abroad), 2, columns) if square else teacher_down
    student_up_shards = chips(student_up)
    up_sent = teacher_shards(teacher_up, up_abroad)
    up_shards = chips(*up_sent)
    part = modulation_part(
        labels, step_index, class_table, teacher_mod, student_mod, up_sent, fast, plane
    )
    own_mods = modulation_sum(part, samples, fast, square, plane)
    mods = modulation_columns(own_mods, columns, col)
    teacher_up_pieces = cores(up_shards)
    down_shards = chips(*after(teacher_shards(teacher_down, down_abroad), up_shards))
    teacher_down_pieces = cores(after(down_shards, mods))
    student_down_shards = chips(after(student_down, own_mods))
    latents, seeds, col, step_index = after((latents, seeds, col, step_index), part)

    if square:
        members = [(0, 0), (0, 1), (2, 0), (2, 1)]
    else:
        members = [(0, flip) for flip in range(columns)]
    chunks = jnp.arange(columns, dtype=jnp.int32) ^ col
    pos = positions(chunks, tokens)
    now = step_index.astype(F32) / STEPS
    alpha, sigma = plan(now)
    alpha_mid, sigma_mid = plan(now - 0.5 / STEPS)
    alpha_end, sigma_end = plan(now - 1.0 / STEPS)
    ratio = sigma_end / sigma
    weight = jnp.maximum(alpha * alpha / (sigma * sigma), 1.0)
    push = -2.0 * sigma * weight / batch_total
    values = [alpha, sigma, alpha_mid, sigma_mid, alpha_end, sigma_end, ratio, alpha_end - ratio * alpha, push]
    lane = lax.broadcasted_iota(jnp.int32, (samples, len(values)), 1)
    coefs = jnp.zeros((samples, len(values)), F32)
    for place_at, value in enumerate(values):
        coefs = jnp.where(lane == place_at, value[:, None], coefs)
    clean = latents.reshape(samples, columns, tokens, PATCH)
    clean = jnp.take(jnp.transpose(clean, (1, 0, 3, 2)), chunks, axis=0)
    token = chunks[:, None, None, None] * tokens + jnp.arange(tokens, dtype=jnp.int32)
    places = token * PATCH + jnp.arange(PATCH, dtype=jnp.int32)[None, None, :, None]
    shaped = (1, samples, 1, 1)
    noisy = alpha.reshape(shaped) * clean + sigma.reshape(shaped) * noise_at(
        seeds.reshape(shaped), places
    )

    def share(parts, flips):
        return [parts[0]] + [
            swap_both(part, flip, plane, columns) for part, flip in zip(parts[1:], flips[1:])
        ]

    def teach(state, first_mod):
        return forward(
            order, state, teacher_patch, teacher_pos, mods, teacher_up_pieces, teacher_down_pieces,
            first_mod, False, 2 if square else 0,
        )

    teacher_pos, teacher_noisy = pos, noisy
    if square:
        near = noisy[:2]
        teacher_noisy = jnp.concatenate([near, swap_plane(near, 2, plane)], axis=0)
        teacher_pos = (jnp.concatenate([pos[0][:2], pos[0][:2]], axis=0), pos[1])
    line = [(0, flip) for flip in range(columns)]
    parts = teach(teacher_noisy, 0)
    first = share(parts, members)
    student_up_pieces = cores(after(student_up_shards, parts))
    student_down_pieces = cores(after(student_down_shards, parts))
    saved = forward(order, noisy, student_patch, pos, mods, student_up_pieces, student_down_pieces, 6, True)
    halfway = middle(coefs, noisy[0], teacher_patch, pos, mods, teacher_out, after(first, saved))
    half_all = jnp.stack([halfway] + [swap_both(halfway, flip, plane, columns) for flip in members[1:]], axis=0)
    student_parts = after(saved[:columns], half_all)
    second = share(teach(half_all, 3), members)
    student = share(student_parts, line)
    act, pre, hidden = saved[columns:]
    back = last(
        coefs,
        noisy[0],
        halfway,
        teacher_patch,
        student_patch,
        pos,
        mods,
        teacher_out,
        student_out,
        second,
        student,
    )
    backs = spread_col(back, columns)

    def pair_sum(blocks):
        if not fast:
            return blocks[0]
        mine, other = blocks
        return mine + swap_plane(other, 1, plane)

    def chip_sum(pair):
        if not fast:
            return lax.psum_scatter(pair, PLANE, scatter_dimension=0, tiled=True)
        total = pair[0]
        for flip in range(1, plane // 2):
            total = total + swap_plane(pair[flip].astype(BF16), 2 * flip, plane).astype(F32)
        return total

    down_blocks = weight_grad(order, backs, hidden, count)
    back_pre = back_through(order, backs, after(pre, down_blocks), student_down_pieces)
    down_pair = pair_sum(down_blocks)
    up_blocks = weight_grad(order, [after(act, down_pair)], back_pre, count)
    up_gradient = chip_sum(pair_sum(up_blocks))
    down_gradient = chip_sum(down_pair)
    return (up_gradient, down_gradient)


def solution(mesh):
    rows = P(("dp", "row"), "col")
    mod = P(("dp", "row"), None, "col")
    batch = P(("dp", "row"))
    placed = (
        P(("dp", "row"), None, None),
        batch,
        batch,
        batch,
        P(),
        P(),
        mod,
        rows,
        rows,
        P(),
        P(),
        mod,
        rows,
        rows,
        P(),
    )

    return jax.shard_map(body, mesh=mesh, in_specs=placed, out_specs=(rows, rows), check_vma=False)
```

```python
import functools
import math

import jax
import jax.numpy as jnp
from jax import lax
from jax.experimental import pallas as pl
from jax.experimental.pallas import tpu as pltpu
from jax.sharding import PartitionSpec as P


D = 1152
CLASSES = 1000
SEQ = 256
PATCH = 16
STEPS = 8

HALF_PI = 0.5 * math.pi
ROOT_TWO_PI = math.sqrt(2.0 / math.pi)
PLANE = ("dp", "row")
F32 = jnp.float32
BF16 = jnp.bfloat16
VMEM_LIMIT = 30 * 1024 * 1024


def plan(times):
    return (jnp.cos(HALF_PI * times), jnp.sin(HALF_PI * times))


def mixing(value):
    amount = jnp.int32(16)
    value = value ^ lax.shift_right_logical(value, amount)
    value = value * 73244475
    value = value ^ lax.shift_right_logical(value, amount)
    value = value * 73244475
    value = value ^ lax.shift_right_logical(value, amount)
    return value


def noise_at(seeds, places):
    mixed = mixing(seeds * 1103515245 + places * 40503 + 12345)
    uniform = (lax.shift_right_logical(mixed, jnp.int32(8)).astype(F32) + 0.5) * (1.0 / 16777216.0)
    return math.sqrt(2.0) * lax.erf_inv(2.0 * uniform - 1.0)


def gelu(pre):
    inner = ROOT_TWO_PI * (pre + 0.044715 * (pre * pre * pre))
    return pre * (0.5 * (1.0 + jnp.tanh(inner)))


def gelu_slope(pre):
    inner = ROOT_TWO_PI * (pre + 0.044715 * pre * pre * pre)
    tangent = jnp.tanh(inner)
    return 0.5 * (1.0 + tangent) + 0.5 * pre * (1.0 - tangent * tangent) * ROOT_TWO_PI * (
        1.0 + 3.0 * 0.044715 * pre * pre
    )


def layer_norm(values):
    center = values - jnp.mean(values, axis=-1, keepdims=True)
    spread = jnp.mean(center * center, axis=-1, keepdims=True)
    reciprocal = lax.rsqrt(spread + 1e-06)
    return (center * reciprocal, reciprocal)


def dot(left, right, dims):
    return lax.dot_general(left, right, (dims, ((), ())), preferred_element_type=F32)


def upright(values):
    tokens = values.shape[1]
    eye = (
        lax.broadcasted_iota(jnp.int32, (tokens, tokens), 0)
        == lax.broadcasted_iota(jnp.int32, (tokens, tokens), 1)
    ).astype(F32).astype(BF16)
    return dot(eye, values.astype(BF16), ((1,), (1,))).astype(BF16)


def place(base, down, across):
    side = across.shape[0]
    parts = []
    for row in range(base.shape[0] // side):
        parts.append(base[row * side : (row + 1) * side] + (down[row : row + 1] + across))
    return jnp.concatenate(parts, axis=0)


def load_pieces(order, pieces, panel, sem):
    copies = []
    for spot, piece in enumerate(pieces):
        rows = piece.shape[0]
        start = pl.multiple_of(order[spot], 16) if len(pieces) > 1 else 0
        copies.append(pltpu.make_async_copy(piece, panel.at[pl.ds(start, rows), :], sem.at[spot]))
    for copy in copies:
        copy.start()
    return copies


def forward_kernel(pieces, first_mod, save, per_set, *refs):
    order, state, patch, down_pos, across, mods = refs[:6]
    refs = refs[6:]
    up_pieces, down_pieces, refs = refs[:pieces], refs[pieces : 2 * pieces], refs[2 * pieces :]
    groups, samples, _, tokens = state.shape
    outs, refs = refs[:groups], refs[groups:]
    if save:
        act, pre_out, hidden = refs[:3]
        refs = refs[3:]
        up, down, up_sem, down_sem = refs
    else:
        act, hidden, up, down, up_sem, down_sem = refs
    up_copies = load_pieces(order, up_pieces, up, up_sem)
    down_copies = load_pieces(order, down_pieces, down, down_sem)

    def embed(group, carry):
        for sample in range(samples):
            base = dot(upright(state[group, sample]), patch[...], ((1,), (0,)))
            base = place(base, down_pos[group], across[...])
            normed, _ = layer_norm(base)
            spot = sample * 9 + first_mod
            if per_set:
                abroad = samples * 9 + sample * 4 + first_mod // 3 * 2
                spot = jnp.where(group < per_set, spot, abroad)
            shift = mods[pl.ds(spot, 1), :]
            scale = mods[pl.ds(spot + 1, 1), :]
            row = pl.multiple_of((group * samples + sample) * tokens, tokens)
            act[pl.ds(row, tokens), :] = (normed * (1.0 + scale) + shift).astype(BF16)
        return carry

    lax.fori_loop(0, groups, embed, 0)
    for copy in up_copies:
        copy.wait()
    block = samples * tokens
    halves = 2 if groups % 2 == 0 else 1
    tall = groups // halves * block

    def first(step, carry):
        at = pl.multiple_of(step * tall, tall)
        pre = dot(act[pl.ds(at, tall), :], up[...], ((1,), (0,)))
        if save:
            pre_out[pl.ds(at, tall), :] = pre
        hidden[pl.ds(at, tall), :] = gelu(pre).astype(BF16)
        return carry

    lax.fori_loop(0, halves, first, 0)
    for copy in down_copies:
        copy.wait()
    part = dot(hidden[...], down[...], ((1,), (1,))).astype(BF16)
    for group in range(groups):
        outs[group][...] = part[group * block : (group + 1) * block]


def full(memory_space=pltpu.VMEM):
    return pl.BlockSpec(memory_space=memory_space)


def forward(order, state, patch, pos, mods, up_pieces, down_pieces, first_mod, save, per_set=0):
    groups, samples, _, tokens = state.shape
    count = len(up_pieces)
    total = groups * samples * tokens
    features = patch.shape[1]
    width = up_pieces[0].shape[1]
    out_shape = [jax.ShapeDtypeStruct((samples * tokens, features), BF16)] * groups
    scratch = [
        pltpu.VMEM((features, width), BF16),
        pltpu.VMEM((features, width), BF16),
        pltpu.SemaphoreType.DMA((count,)),
        pltpu.SemaphoreType.DMA((count,)),
    ]
    if save:
        out_shape = out_shape + [
            jax.ShapeDtypeStruct((total, features), BF16),
            jax.ShapeDtypeStruct((total, width), F32),
            jax.ShapeDtypeStruct((total, width), BF16),
        ]
    else:
        scratch = [pltpu.VMEM((total, features), BF16), pltpu.VMEM((total, width), BF16)] + scratch
    return pl.pallas_call(
        functools.partial(forward_kernel, count, first_mod, save, per_set),
        out_shape=out_shape,
        in_specs=[full(pltpu.SMEM)] + [full()] * 5 + [full(pltpu.HBM)] * (2 * count),
        out_specs=[full()] * len(out_shape),
        scratch_shapes=scratch,
        compiler_params=pltpu.CompilerParams(vmem_limit_bytes=VMEM_LIMIT),
        cost_estimate=pl.CostEstimate(
            flops=4 * total * features * width, bytes_accessed=8 * features * width, transcendentals=total * width
        ),
    )(order, state, patch, *pos, mods, *up_pieces, *down_pieces)


def settle(parts, state, patch, down_pos, across, mods, out, gate_at, sample):
    tokens = state.shape[2]
    rows = slice(sample * tokens, (sample + 1) * tokens)
    mixed = parts[0][rows].astype(F32)
    for part in parts[1:]:
        mixed = mixed + part[rows].astype(F32)
    gate_row = sample * 9 + gate_at
    gate = mods[gate_row : gate_row + 1, :]
    base = dot(upright(state[sample]), patch[...], ((1,), (0,)))
    base = place(base, down_pos[0], across[...])
    final, reciprocal = layer_norm(base + gate * mixed)
    velocity = dot(out[...], final.astype(BF16), ((1,), (1,)))
    return velocity, final, reciprocal, gate


def middle_kernel(groups, *refs):
    coefs, state, patch, down_pos, across, mods, out = refs[:7]
    parts, halfway = refs[7 : 7 + groups], refs[7 + groups]
    for sample in range(state.shape[0]):
        velocity, _, _, _ = settle(parts, state, patch, down_pos, across, mods, out, 2, sample)
        noisy = state[sample]
        alpha, sigma = coefs[sample, 0], coefs[sample, 1]
        alpha_mid, sigma_mid = coefs[sample, 2], coefs[sample, 3]
        first_x = alpha * noisy - sigma * velocity
        halfway[sample] = alpha_mid * first_x + sigma_mid * (noisy - alpha * first_x) / sigma


def middle(coefs, state, patch, pos, mods, out, parts):
    groups = len(parts)
    return pl.pallas_call(
        functools.partial(middle_kernel, groups),
        out_shape=jax.ShapeDtypeStruct(state.shape, F32),
        in_specs=[full(pltpu.SMEM)] + [full()] * (6 + groups),
        out_specs=full(),
        compiler_params=pltpu.CompilerParams(vmem_limit_bytes=VMEM_LIMIT),
        cost_estimate=pl.CostEstimate(flops=10**9, bytes_accessed=2 * 10**6, transcendentals=0),
        name="middle",
    )(coefs, state, patch, *pos, mods, out, *parts)


def last_kernel(groups, *refs):
    coefs, noisy_ref, half_ref, t_patch, s_patch, down_pos, across, mods, t_out, s_out = refs[:10]
    refs = refs[10:]
    teacher, student, back = refs[:groups], refs[groups : 2 * groups], refs[2 * groups]
    samples, _, tokens = noisy_ref.shape
    for sample in range(samples):
        second_v, _, _, _ = settle(
            teacher, half_ref, t_patch, down_pos, across, mods, t_out, 5, sample
        )
        student_v, final, reciprocal, gate = settle(
            student, noisy_ref, s_patch, down_pos, across, mods, s_out, 8, sample
        )
        noisy, halfway = noisy_ref[sample], half_ref[sample]
        alpha, sigma = coefs[sample, 0], coefs[sample, 1]
        alpha_mid, sigma_mid = coefs[sample, 2], coefs[sample, 3]
        alpha_end, sigma_end = coefs[sample, 4], coefs[sample, 5]
        ratio, gap, push = coefs[sample, 6], coefs[sample, 7], coefs[sample, 8]
        second_x = alpha_mid * halfway - sigma_mid * second_v
        landing = alpha_end * second_x + sigma_end * (halfway - alpha_mid * second_x) / sigma_mid
        target = (landing - ratio * noisy) / gap
        student_x = alpha * noisy - sigma * student_v
        back_velocity = push * (student_x - target)
        high = back_velocity.astype(BF16)
        rest = back_velocity - high.astype(F32)
        mid = rest.astype(BF16)
        low = (rest - mid.astype(F32)).astype(BF16)
        back_final = dot(upright(low), s_out[...], ((1,), (0,)))
        back_final = back_final + dot(upright(mid), s_out[...], ((1,), (0,)))
        back_final = back_final + dot(upright(high), s_out[...], ((1,), (0,)))
        centre = jnp.mean(back_final, axis=-1, keepdims=True)
        along = jnp.mean(back_final * final, axis=-1, keepdims=True)
        back[sample * tokens : (sample + 1) * tokens, :] = (
            gate * (reciprocal * (back_final - centre - final * along))
        ).astype(BF16)


def last(coefs, noisy, halfway, t_patch, s_patch, pos, mods, t_out, s_out, teacher, student):
    groups = len(teacher)
    samples, _, tokens = noisy.shape
    return pl.pallas_call(
        functools.partial(last_kernel, groups),
        out_shape=jax.ShapeDtypeStruct((samples * tokens, t_out.shape[1]), BF16),
        in_specs=[full(pltpu.SMEM)] + [full()] * (9 + 2 * groups),
        out_specs=full(),
        compiler_params=pltpu.CompilerParams(vmem_limit_bytes=VMEM_LIMIT),
        cost_estimate=pl.CostEstimate(flops=2 * 10**9, bytes_accessed=4 * 10**6, transcendentals=0),
        name="last",
    )(coefs, noisy, halfway, t_patch, s_patch, *pos, mods, t_out, s_out, *teacher, *student)


def store_blocks(order, grad, blocks, sem):
    copies = []
    if len(blocks) == 1:
        copies.append(pltpu.make_async_copy(grad, blocks[0], sem.at[0]))
    else:
        mine, other = blocks
        count, rows = mine.shape[0], mine.shape[1]
        for spot in range(2 * count):
            start = pl.multiple_of(order[spot], 8)
            target = (mine, other)[spot % 2].at[spot // 2]
            copies.append(pltpu.make_async_copy(grad.at[pl.ds(start, rows), :], target, sem.at[spot]))
    for copy in copies:
        copy.start()
    for copy in copies:
        copy.wait()


def gather_rows(parts, whole):
    at = 0
    for part in parts:
        rows = part.shape[0]
        whole[at : at + rows, :] = part[...]
        at += rows


def weight_grad_kernel(lefts, rights, start, more, outs, *refs):
    order, refs = refs[0], refs[1:]
    left_parts, refs = refs[:lefts], refs[lefts:]
    right_parts, refs = refs[:rights], refs[rights:]
    so_far, refs = (refs[0], refs[1:]) if more else (None, refs)
    blocks, (left, right, grad, sem) = refs[:-4], refs[-4:]
    gather_rows(left_parts, left)
    total = left.shape[0]
    if rights == 1:
        values = right_parts[0][start : start + total, :]
    else:
        gather_rows(right_parts, right)
        values = right[...]
    target = grad if outs else blocks[0]
    part = dot(left[...], values, ((0,), (0,)))
    target[...] = part + so_far[...] if more else part
    if outs:
        store_blocks(order, grad, blocks, sem)


def back_pre_kernel(groups, pieces, start, *refs):
    order, refs = refs[0], refs[1:]
    backs, pre, refs = refs[:groups], refs[groups], refs[groups + 1 :]
    down_pieces, (back_pre, back, down, sem) = refs[:pieces], refs[pieces:]
    copies = load_pieces(order, down_pieces, down, sem)
    gather_rows(backs, back)
    for copy in copies:
        copy.wait()
    rows = back.shape[0]
    back_hidden = dot(back[...], down[...], ((1,), (0,)))
    back_pre[...] = (back_hidden * gelu_slope(pre[start : start + rows, :])).astype(BF16)


def block_shapes(count, features, width):
    if count == 1:
        return [jax.ShapeDtypeStruct((features, width), F32)]
    return [jax.ShapeDtypeStruct((count // 2, features // count, width), F32)] * 2


def weight_grad(order, lefts, rights, count, start=0, so_far=None, whole=False):
    features, width = lefts[0].shape[1], rights[0].shape[1]
    total = sum(part.shape[0] for part in lefts)
    shapes = [jax.ShapeDtypeStruct((features, width), F32)] if whole else block_shapes(count, features, width)
    outs = 0 if whole else len(shapes)
    more = [] if so_far is None else [so_far]
    vmem = len(lefts) + len(rights) + len(more)
    return pl.pallas_call(
        functools.partial(weight_grad_kernel, len(lefts), len(rights), start, bool(more), outs),
        out_shape=shapes,
        in_specs=[full(pltpu.SMEM)] + [full()] * vmem,
        out_specs=[full() if whole else full(pl.ANY)] * len(shapes),
        scratch_shapes=[
            pltpu.VMEM((total, features), BF16),
            pltpu.VMEM((total if len(rights) > 1 else 16, width), BF16),
            pltpu.VMEM((8, width) if whole else (features, width), F32),
            pltpu.SemaphoreType.DMA((count,)),
        ],
        compiler_params=pltpu.CompilerParams(vmem_limit_bytes=VMEM_LIMIT),
        cost_estimate=pl.CostEstimate(
            flops=2 * total * features * width, bytes_accessed=8 * features * width, transcendentals=0
        ),
    )(order, *lefts, *rights, *more)


def back_through(order, backs, pre, down_pieces, start):
    features = backs[0].shape[1]
    width = pre.shape[1]
    total = sum(back.shape[0] for back in backs)
    pieces = len(down_pieces)
    return pl.pallas_call(
        functools.partial(back_pre_kernel, len(backs), pieces, start),
        out_shape=jax.ShapeDtypeStruct((total, width), BF16),
        in_specs=[full(pltpu.SMEM)] + [full()] * (len(backs) + 1) + [full(pltpu.HBM)] * pieces,
        out_specs=full(),
        scratch_shapes=[
            pltpu.VMEM((total, features), BF16),
            pltpu.VMEM((features, width), BF16),
            pltpu.SemaphoreType.DMA((pieces,)),
        ],
        compiler_params=pltpu.CompilerParams(vmem_limit_bytes=VMEM_LIMIT),
        cost_estimate=pl.CostEstimate(
            flops=2 * total * features * width, bytes_accessed=8 * features * width, transcendentals=total * width
        ),
    )(order, *backs, pre, *down_pieces)


def after(value, earlier):
    return lax.optimization_barrier((value, earlier))[0]


def swap_plane(value, flip, size):
    return lax.ppermute(value, PLANE, [(spot, spot ^ flip) for spot in range(size)])


def swap_col(value, flip, size):
    return lax.ppermute(value, "col", [(spot, spot ^ flip) for spot in range(size)])


def swap_both(value, flip, plane, columns):
    pairs = []
    for spot in range(plane):
        for col in range(columns):
            pairs.append((spot * columns + col, (spot ^ flip[0]) * columns + (col ^ flip[1])))
    return lax.ppermute(value, ("dp", "row", "col"), pairs)


def chips_of_plane(even, odd, size):
    return [even] + [swap_plane((even, odd)[flip % 2], 2 * flip, size) for flip in range(1, size // 2)]


def both_cores(shards, size):
    pieces = []
    for shard in shards:
        pieces += [shard, swap_plane(shard, 1, size)]
    return pieces


def spread_col(value, size):
    return [value] + [swap_col(value, flip, size) for flip in range(1, size)]


def condition(times, embedded, offset, rows):
    half = D // 2
    places = offset + jnp.arange(rows, dtype=jnp.int32)
    low = places < half
    power = jnp.where(low, places, places - half).astype(F32)
    freqs = jnp.exp(-math.log(10000.0) * power / half)
    angle = (1000.0 * times)[:, None] * freqs[None, :]
    features = jnp.where(low[None, :], jnp.cos(angle), jnp.sin(angle))
    return jax.nn.silu(embedded + features).astype(BF16)


def modulation_part(labels, step_index, class_table, teacher_mod, student_mod, earlier, fast, plane):
    rows = teacher_mod.shape[0]
    packed = labels * 16 + step_index
    if fast:
        others = [swap_plane(packed, flip, plane) for flip in range(1, plane)]
        everyone = jnp.concatenate([packed] + others, axis=0)
    else:
        everyone = lax.all_gather(packed, PLANE, axis=0, tiled=True)
    everyone = after(everyone, earlier)
    all_labels, all_steps = everyone // 16, everyone % 16
    all_now = all_steps.astype(F32) / STEPS
    offset = lax.axis_index(PLANE) * rows
    table = lax.dynamic_slice_in_dim(class_table, offset, rows, 1)
    onehot = (all_labels[:, None] == jnp.arange(CLASSES, dtype=jnp.int32)[None, :]).astype(BF16)
    embedded = jnp.dot(onehot, table, preferred_element_type=F32)
    rows_now = condition(all_now, embedded, offset, rows)
    rows_mid = condition(all_now - 0.5 / STEPS, embedded, offset, rows)
    count = rows_now.shape[0]
    share = teacher_mod.shape[2]
    teacher_flat = teacher_mod.reshape(rows, 3 * share)
    student_flat = student_mod.reshape(rows, 3 * share)
    teacher_part = jnp.dot(
        jnp.concatenate([rows_now, rows_mid], axis=0), teacher_flat, preferred_element_type=F32
    )
    student_part = jnp.dot(rows_now, student_flat, preferred_element_type=F32)
    return jnp.concatenate([teacher_part[:count], teacher_part[count:], student_part], axis=1)


def modulation_sum(part, samples, fast, square, plane):
    if not fast:
        return lax.psum_scatter(part, PLANE, scatter_dimension=0, tiled=True)[None]
    part = part.reshape(plane // 2, 2, samples, part.shape[1])
    pair = part[:, 0] + swap_plane(part[:, 1], 1, plane)
    sets = 2 if square else 1
    own = jnp.stack([pair[other] for other in range(sets)], axis=0)
    for flip in range(1, plane // 2):
        sent = jnp.stack([pair[flip ^ other] for other in range(sets)], axis=0)
        own = own + swap_plane(sent, 2 * flip, plane)
    return own


def modulation_columns(own, columns, col):
    sets, samples = own.shape[:2]
    share = own.shape[2] // 9
    rows = own.reshape(sets, samples, 9, share)
    packed = [rows[0].reshape(samples * 9, share)]
    for other in range(1, sets):
        packed.append(jnp.concatenate([rows[other, :, 0:2], rows[other, :, 3:5]], axis=1).reshape(samples * 4, share))
    packed = jnp.concatenate(packed, axis=0)
    gathered = spread_col(packed, columns)
    ordered = []
    for place_at in range(columns):
        piece = gathered[place_at]
        for other in range(1, columns):
            piece = jnp.where(col == other, gathered[place_at ^ other], piece)
        ordered.append(piece)
    return jnp.concatenate(ordered, axis=1)


def positions(chunks, tokens):
    quarter = D // 4
    omega = 1.0 / 10000.0 ** (jnp.arange(quarter, dtype=F32) / quarter)
    side = math.isqrt(SEQ)
    span = tokens // side
    angle = jnp.arange(side, dtype=F32)[:, None] * omega[None, :]
    across = jnp.concatenate([jnp.zeros((side, D // 2), F32), jnp.sin(angle), jnp.cos(angle)], axis=1)
    grid_rows = chunks[:, None] * span + jnp.arange(span, dtype=jnp.int32)
    turn = grid_rows.astype(F32)[:, :, None] * omega
    down = jnp.concatenate(
        [jnp.sin(turn), jnp.cos(turn), jnp.zeros((chunks.shape[0], span, D // 2), F32)], axis=2
    )
    return down, across


def body(
    latents,
    labels,
    step_index,
    seeds,
    class_table,
    teacher_patch,
    teacher_mod,
    teacher_up,
    teacher_down,
    teacher_out,
    student_patch,
    student_mod,
    student_up,
    student_down,
    student_out,
):
    samples = latents.shape[0]
    plane = lax.axis_size(PLANE)
    columns = lax.axis_size("col")
    batch_total = samples * plane
    col = lax.axis_index("col")
    spot = lax.axis_index(PLANE)
    rows = teacher_up.shape[0]
    tokens = SEQ // columns
    fast = rows % 16 == 0 and plane <= 8
    count = plane if fast else 1

    order = ((jnp.arange(count, dtype=jnp.int32) ^ spot) * rows).astype(jnp.int32)

    square = fast and columns == 4 and plane >= 4
    odd_chip = (spot // 2) % 2 == 1

    def chips(even, odd=None):
        if fast:
            return chips_of_plane(even, even if odd is None else odd, plane)
        return [lax.all_gather(even, PLANE, axis=0, tiled=True)]

    def cores(shards):
        return both_cores(shards, plane) if fast else shards

    def teacher_shards(shard, abroad):
        if not square:
            return (shard,)
        return jnp.where(odd_chip, abroad, shard), jnp.where(odd_chip, shard, abroad)

    up_abroad = swap_col(teacher_up, 2, columns) if square else teacher_up
    down_abroad = swap_col(after(teacher_down, up_abroad), 2, columns) if square else teacher_down
    student_up_shards = chips(student_up)
    up_sent = teacher_shards(teacher_up, up_abroad)
    up_shards = chips(*up_sent)
    part = modulation_part(
        labels, step_index, class_table, teacher_mod, student_mod, up_sent, fast, plane
    )
    own_mods = modulation_sum(part, samples, fast, square, plane)
    mods = modulation_columns(own_mods, columns, col)
    teacher_up_pieces = cores(up_shards)
    down_shards = chips(*teacher_shards(teacher_down, down_abroad))
    teacher_down_pieces = cores(down_shards)
    student_down_shards = chips(after(student_down, own_mods))
    latents, seeds, col, step_index = after((latents, seeds, col, step_index), part)

    if square:
        members = [(0, 0), (0, 1), (2, 0), (2, 1)]
    else:
        members = [(0, flip) for flip in range(columns)]
    chunks = jnp.arange(columns, dtype=jnp.int32) ^ col
    pos = positions(chunks, tokens)
    now = step_index.astype(F32) / STEPS
    alpha, sigma = plan(now)
    alpha_mid, sigma_mid = plan(now - 0.5 / STEPS)
    alpha_end, sigma_end = plan(now - 1.0 / STEPS)
    ratio = sigma_end / sigma
    weight = jnp.maximum(alpha * alpha / (sigma * sigma), 1.0)
    push = -2.0 * sigma * weight / batch_total
    values = [alpha, sigma, alpha_mid, sigma_mid, alpha_end, sigma_end, ratio, alpha_end - ratio * alpha, push]
    lane = lax.broadcasted_iota(jnp.int32, (samples, len(values)), 1)
    coefs = jnp.zeros((samples, len(values)), F32)
    for place_at, value in enumerate(values):
        coefs = jnp.where(lane == place_at, value[:, None], coefs)
    clean = latents.reshape(samples, columns, tokens, PATCH)
    clean = jnp.take(jnp.transpose(clean, (1, 0, 3, 2)), chunks, axis=0)
    token = chunks[:, None, None, None] * tokens + jnp.arange(tokens, dtype=jnp.int32)
    places = token * PATCH + jnp.arange(PATCH, dtype=jnp.int32)[None, None, :, None]
    shaped = (1, samples, 1, 1)
    noisy = alpha.reshape(shaped) * clean + sigma.reshape(shaped) * noise_at(
        seeds.reshape(shaped), places
    )

    def share(parts, flips):
        return [parts[0]] + [
            swap_both(part, flip, plane, columns) for part, flip in zip(parts[1:], flips[1:])
        ]

    def teach(state, first_mod):
        return forward(
            order, state, teacher_patch, teacher_pos, mods, teacher_up_pieces, teacher_down_pieces,
            first_mod, False, 2 if square else 0,
        )

    student_up_pieces = cores(after(student_up_shards, down_shards))
    teacher_pos, teacher_noisy = pos, noisy
    if square:
        near = noisy[:2]
        teacher_noisy = jnp.concatenate([near, swap_plane(near, 2, plane)], axis=0)
        teacher_pos = (jnp.concatenate([pos[0][:2], pos[0][:2]], axis=0), pos[1])
    line = [(0, flip) for flip in range(columns)]
    parts = teach(teacher_noisy, 0)
    first = share(parts, members)
    student_down_pieces = cores(after(student_down_shards, parts))
    saved = forward(order, noisy, student_patch, pos, mods, student_up_pieces, student_down_pieces, 6, True)
    halfway = middle(coefs, noisy[0], teacher_patch, pos, mods, teacher_out, after(first, saved))
    half_all = jnp.stack([halfway] + [swap_both(halfway, flip, plane, columns) for flip in members[1:]], axis=0)
    early = swap_both(saved[2 % columns], line[2 % columns], plane, columns)
    student = [saved[0], early] + [
        swap_both(after(saved[spot], half_all), line[spot], plane, columns)
        for spot in range(1, columns)
        if spot != 2 % columns
    ]
    second = share(teach(half_all, 3), members)
    act, pre, hidden = saved[columns:]
    back = last(
        coefs,
        noisy[0],
        halfway,
        teacher_patch,
        student_patch,
        pos,
        mods,
        teacher_out,
        student_out,
        second,
        student,
    )
    if columns == 4:
        across = swap_col(back, 2, columns)
        beside = swap_col(back, 1, columns)
        backs = [back, beside, across, swap_col(across, 1, columns)]
    else:
        backs = spread_col(back, columns)

    def pair_sum(blocks):
        if not fast:
            return blocks[0]
        mine, other = blocks
        return mine + swap_plane(other, 1, plane)

    def chip_sum(pair):
        if not fast:
            return lax.psum_scatter(pair, PLANE, scatter_dimension=0, tiled=True)
        total = pair[0]
        for flip in range(1, plane // 2):
            total = total + swap_plane(pair[flip].astype(BF16), 2 * flip, plane).astype(F32)
        return total

    split = (columns - 1) * back.shape[0]
    (down_early,) = weight_grad(order, backs[:-1], [hidden], count, whole=True)
    pre_early = back_through(order, backs[:-1], pre, student_down_pieces, 0)
    down_blocks = weight_grad(order, after(backs[-1:], pre_early), [hidden], count, split, down_early)
    pre_late = back_through(order, backs[-1:], after(pre, down_blocks), student_down_pieces, split)
    down_pair = pair_sum(down_blocks)
    up_blocks = weight_grad(order, [after(act, down_pair)], [pre_early, pre_late], count)
    down_gradient = chip_sum(down_pair)
    up_gradient = chip_sum(pair_sum(up_blocks))
    return (up_gradient, down_gradient)


def solution(mesh):
    rows = P(("dp", "row"), "col")
    mod = P(("dp", "row"), None, "col")
    batch = P(("dp", "row"))
    placed = (
        P(("dp", "row"), None, None),
        batch,
        batch,
        batch,
        P(),
        P(),
        mod,
        rows,
        rows,
        P(),
        P(),
        mod,
        rows,
        rows,
        P(),
    )

    return jax.shard_map(body, mesh=mesh, in_specs=placed, out_specs=(rows, rows), check_vma=False)
```

```python
import functools
import math

import jax
import jax.numpy as jnp
from jax import lax
from jax.experimental import pallas as pl
from jax.experimental.pallas import tpu as pltpu
from jax.sharding import PartitionSpec as P


D = 1152
CLASSES = 1000
SEQ = 256
PATCH = 16
STEPS = 8

HALF_PI = 0.5 * math.pi
ROOT_TWO_PI = math.sqrt(2.0 / math.pi)
PLANE = ("dp", "row")
F32 = jnp.float32
BF16 = jnp.bfloat16
VMEM_LIMIT = 30 * 1024 * 1024


def plan(times):
    return (jnp.cos(HALF_PI * times), jnp.sin(HALF_PI * times))


def mixing(value):
    amount = jnp.int32(16)
    value = value ^ lax.shift_right_logical(value, amount)
    value = value * 73244475
    value = value ^ lax.shift_right_logical(value, amount)
    value = value * 73244475
    value = value ^ lax.shift_right_logical(value, amount)
    return value


def noise_at(seeds, places):
    mixed = mixing(seeds * 1103515245 + places * 40503 + 12345)
    uniform = (lax.shift_right_logical(mixed, jnp.int32(8)).astype(F32) + 0.5) * (1.0 / 16777216.0)
    return math.sqrt(2.0) * lax.erf_inv(2.0 * uniform - 1.0)


def gelu(pre):
    inner = ROOT_TWO_PI * (pre + 0.044715 * (pre * pre * pre))
    return pre * (0.5 * (1.0 + jnp.tanh(inner)))


def gelu_slope(pre):
    inner = ROOT_TWO_PI * (pre + 0.044715 * pre * pre * pre)
    tangent = jnp.tanh(inner)
    return 0.5 * (1.0 + tangent) + 0.5 * pre * (1.0 - tangent * tangent) * ROOT_TWO_PI * (
        1.0 + 3.0 * 0.044715 * pre * pre
    )


def layer_norm(values):
    center = values - jnp.mean(values, axis=-1, keepdims=True)
    spread = jnp.mean(center * center, axis=-1, keepdims=True)
    reciprocal = lax.rsqrt(spread + 1e-06)
    return (center * reciprocal, reciprocal)


def dot(left, right, dims):
    return lax.dot_general(left, right, (dims, ((), ())), preferred_element_type=F32)


def upright(values):
    tokens = values.shape[1]
    eye = (
        lax.broadcasted_iota(jnp.int32, (tokens, tokens), 0)
        == lax.broadcasted_iota(jnp.int32, (tokens, tokens), 1)
    ).astype(F32).astype(BF16)
    return dot(eye, values.astype(BF16), ((1,), (1,))).astype(BF16)


def place(base, down, across):
    side = across.shape[0]
    parts = []
    for row in range(base.shape[0] // side):
        parts.append(base[row * side : (row + 1) * side] + (down[row : row + 1] + across))
    return jnp.concatenate(parts, axis=0)


def load_pieces(order, pieces, panel, sem):
    copies = []
    for spot, piece in enumerate(pieces):
        rows = piece.shape[0]
        start = pl.multiple_of(order[spot], 16) if len(pieces) > 1 else 0
        copies.append(pltpu.make_async_copy(piece, panel.at[pl.ds(start, rows), :], sem.at[spot]))
    for copy in copies:
        copy.start()
    return copies


def forward_kernel(pieces, first_mod, save, per_set, *refs):
    order, state, patch, down_pos, across, mods = refs[:6]
    refs = refs[6:]
    up_pieces, down_pieces, refs = refs[:pieces], refs[pieces : 2 * pieces], refs[2 * pieces :]
    groups, samples, _, tokens = state.shape
    outs, refs = refs[:groups], refs[groups:]
    if save:
        act, pre_out, hidden = refs[:3]
        refs = refs[3:]
        up, down, up_sem, down_sem = refs
    else:
        act, hidden, up, down, up_sem, down_sem = refs
    up_copies = load_pieces(order, up_pieces, up, up_sem)
    down_copies = load_pieces(order, down_pieces, down, down_sem)

    def embed(group, carry):
        for sample in range(samples):
            base = dot(upright(state[group, sample]), patch[...], ((1,), (0,)))
            base = place(base, down_pos[group], across[...])
            normed, _ = layer_norm(base)
            spot = sample * (mods.shape[0] // samples) + first_mod
            if per_set:
                abroad = spot - first_mod + 9 + first_mod // 3 * 2
                spot = jnp.where(group < per_set, spot, abroad)
            shift = mods[pl.ds(spot, 1), :]
            scale = mods[pl.ds(spot + 1, 1), :]
            row = pl.multiple_of((group * samples + sample) * tokens, tokens)
            act[pl.ds(row, tokens), :] = (normed * (1.0 + scale) + shift).astype(BF16)
        return carry

    lax.fori_loop(0, groups, embed, 0)
    for copy in up_copies:
        copy.wait()
    block = samples * tokens
    halves = 2 if groups % 2 == 0 else 1
    tall = groups // halves * block

    def first(step, carry):
        at = pl.multiple_of(step * tall, tall)
        pre = dot(act[pl.ds(at, tall), :], up[...], ((1,), (0,)))
        if save:
            pre_out[pl.ds(at, tall), :] = pre
        hidden[pl.ds(at, tall), :] = gelu(pre).astype(BF16)
        return carry

    lax.fori_loop(0, halves, first, 0)
    for copy in down_copies:
        copy.wait()
    part = dot(hidden[...], down[...], ((1,), (1,))).astype(BF16)
    for group in range(groups):
        outs[group][...] = part[group * block : (group + 1) * block]


def full(memory_space=pltpu.VMEM):
    return pl.BlockSpec(memory_space=memory_space)


def forward(order, state, patch, pos, mods, up_pieces, down_pieces, first_mod, save, per_set=0):
    groups, samples, _, tokens = state.shape
    count = len(up_pieces)
    total = groups * samples * tokens
    features = patch.shape[1]
    width = up_pieces[0].shape[1]
    out_shape = [jax.ShapeDtypeStruct((samples * tokens, features), BF16)] * groups
    scratch = [
        pltpu.VMEM((features, width), BF16),
        pltpu.VMEM((features, width), BF16),
        pltpu.SemaphoreType.DMA((count,)),
        pltpu.SemaphoreType.DMA((count,)),
    ]
    if save:
        out_shape = out_shape + [
            jax.ShapeDtypeStruct((total, features), BF16),
            jax.ShapeDtypeStruct((total, width), F32),
            jax.ShapeDtypeStruct((total, width), BF16),
        ]
    else:
        scratch = [pltpu.VMEM((total, features), BF16), pltpu.VMEM((total, width), BF16)] + scratch
    return pl.pallas_call(
        functools.partial(forward_kernel, count, first_mod, save, per_set),
        out_shape=out_shape,
        in_specs=[full(pltpu.SMEM)] + [full()] * 5 + [full(pltpu.HBM)] * (2 * count),
        out_specs=[full()] * len(out_shape),
        scratch_shapes=scratch,
        compiler_params=pltpu.CompilerParams(vmem_limit_bytes=VMEM_LIMIT),
        cost_estimate=pl.CostEstimate(
            flops=4 * total * features * width, bytes_accessed=8 * features * width, transcendentals=total * width
        ),
    )(order, state, patch, *pos, mods, *up_pieces, *down_pieces)


def settle(parts, state, patch, down_pos, across, mods, out, gate_at, sample):
    tokens = state.shape[2]
    rows = slice(sample * tokens, (sample + 1) * tokens)
    mixed = parts[0][rows].astype(F32)
    for part in parts[1:]:
        mixed = mixed + part[rows].astype(F32)
    gate_row = sample * (mods.shape[0] // state.shape[0]) + gate_at
    gate = mods[gate_row : gate_row + 1, :]
    base = dot(upright(state[sample]), patch[...], ((1,), (0,)))
    base = place(base, down_pos[0], across[...])
    final, reciprocal = layer_norm(base + gate * mixed)
    velocity = dot(out[...], final.astype(BF16), ((1,), (1,)))
    return velocity, final, reciprocal, gate


def middle_kernel(groups, *refs):
    coefs, state, patch, down_pos, across, mods, out = refs[:7]
    parts, halfway = refs[7 : 7 + groups], refs[7 + groups]
    for sample in range(state.shape[0]):
        velocity, _, _, _ = settle(parts, state, patch, down_pos, across, mods, out, 2, sample)
        noisy = state[sample]
        alpha, sigma = coefs[sample, 0], coefs[sample, 1]
        alpha_mid, sigma_mid = coefs[sample, 2], coefs[sample, 3]
        first_x = alpha * noisy - sigma * velocity
        halfway[sample] = alpha_mid * first_x + sigma_mid * (noisy - alpha * first_x) / sigma


def middle(coefs, state, patch, pos, mods, out, parts):
    groups = len(parts)
    return pl.pallas_call(
        functools.partial(middle_kernel, groups),
        out_shape=jax.ShapeDtypeStruct(state.shape, F32),
        in_specs=[full(pltpu.SMEM)] + [full()] * (6 + groups),
        out_specs=full(),
        compiler_params=pltpu.CompilerParams(vmem_limit_bytes=VMEM_LIMIT),
        cost_estimate=pl.CostEstimate(flops=10**9, bytes_accessed=2 * 10**6, transcendentals=0),
        name="middle",
    )(coefs, state, patch, *pos, mods, out, *parts)


def last_kernel(groups, *refs):
    coefs, noisy_ref, half_ref, t_patch, s_patch, down_pos, across, mods, t_out, s_out = refs[:10]
    refs = refs[10:]
    teacher, student, back = refs[:groups], refs[groups : 2 * groups], refs[2 * groups]
    samples, _, tokens = noisy_ref.shape
    for sample in range(samples):
        second_v, _, _, _ = settle(
            teacher, half_ref, t_patch, down_pos, across, mods, t_out, 5, sample
        )
        student_v, final, reciprocal, gate = settle(
            student, noisy_ref, s_patch, down_pos, across, mods, s_out, 8, sample
        )
        noisy, halfway = noisy_ref[sample], half_ref[sample]
        alpha, sigma = coefs[sample, 0], coefs[sample, 1]
        alpha_mid, sigma_mid = coefs[sample, 2], coefs[sample, 3]
        alpha_end, sigma_end = coefs[sample, 4], coefs[sample, 5]
        ratio, gap, push = coefs[sample, 6], coefs[sample, 7], coefs[sample, 8]
        second_x = alpha_mid * halfway - sigma_mid * second_v
        landing = alpha_end * second_x + sigma_end * (halfway - alpha_mid * second_x) / sigma_mid
        target = (landing - ratio * noisy) / gap
        student_x = alpha * noisy - sigma * student_v
        back_velocity = push * (student_x - target)
        high = back_velocity.astype(BF16)
        rest = back_velocity - high.astype(F32)
        mid = rest.astype(BF16)
        low = (rest - mid.astype(F32)).astype(BF16)
        back_final = dot(upright(low), s_out[...], ((1,), (0,)))
        back_final = back_final + dot(upright(mid), s_out[...], ((1,), (0,)))
        back_final = back_final + dot(upright(high), s_out[...], ((1,), (0,)))
        centre = jnp.mean(back_final, axis=-1, keepdims=True)
        along = jnp.mean(back_final * final, axis=-1, keepdims=True)
        back[sample * tokens : (sample + 1) * tokens, :] = (
            gate * (reciprocal * (back_final - centre - final * along))
        ).astype(BF16)


def last(coefs, noisy, halfway, t_patch, s_patch, pos, mods, t_out, s_out, teacher, student):
    groups = len(teacher)
    samples, _, tokens = noisy.shape
    return pl.pallas_call(
        functools.partial(last_kernel, groups),
        out_shape=jax.ShapeDtypeStruct((samples * tokens, t_out.shape[1]), BF16),
        in_specs=[full(pltpu.SMEM)] + [full()] * (9 + 2 * groups),
        out_specs=full(),
        compiler_params=pltpu.CompilerParams(vmem_limit_bytes=VMEM_LIMIT),
        cost_estimate=pl.CostEstimate(flops=2 * 10**9, bytes_accessed=4 * 10**6, transcendentals=0),
        name="last",
    )(coefs, noisy, halfway, t_patch, s_patch, *pos, mods, t_out, s_out, *teacher, *student)


def store_blocks(order, grad, blocks, sem):
    copies = []
    if len(blocks) == 1:
        copies.append(pltpu.make_async_copy(grad, blocks[0], sem.at[0]))
    else:
        mine, other = blocks
        count, rows = mine.shape[0], mine.shape[1]
        for spot in range(2 * count):
            start = pl.multiple_of(order[spot], 8)
            target = (mine, other)[spot % 2].at[spot // 2]
            copies.append(pltpu.make_async_copy(grad.at[pl.ds(start, rows), :], target, sem.at[spot]))
    for copy in copies:
        copy.start()
    for copy in copies:
        copy.wait()


def gather_rows(parts, whole):
    at = 0
    for part in parts:
        rows = part.shape[0]
        whole[at : at + rows, :] = part[...]
        at += rows


def weight_grad_kernel(lefts, rights, start, more, outs, *refs):
    order, refs = refs[0], refs[1:]
    left_parts, refs = refs[:lefts], refs[lefts:]
    right_parts, refs = refs[:rights], refs[rights:]
    so_far, refs = (refs[0], refs[1:]) if more else (None, refs)
    blocks, (left, right, grad, sem) = refs[:-4], refs[-4:]
    gather_rows(left_parts, left)
    total = left.shape[0]
    if rights == 1:
        values = right_parts[0][start : start + total, :]
    else:
        gather_rows(right_parts, right)
        values = right[...]
    target = grad if outs else blocks[0]
    part = dot(left[...], values, ((0,), (0,)))
    target[...] = part + so_far[...] if more else part
    if outs:
        store_blocks(order, grad, blocks, sem)


def back_pre_kernel(groups, pieces, start, *refs):
    order, refs = refs[0], refs[1:]
    backs, pre, refs = refs[:groups], refs[groups], refs[groups + 1 :]
    down_pieces, (back_pre, back, down, sem) = refs[:pieces], refs[pieces:]
    copies = load_pieces(order, down_pieces, down, sem)
    gather_rows(backs, back)
    for copy in copies:
        copy.wait()
    rows = back.shape[0]
    back_hidden = dot(back[...], down[...], ((1,), (0,)))
    back_pre[...] = (back_hidden * gelu_slope(pre[start : start + rows, :])).astype(BF16)


def block_shapes(count, features, width):
    if count == 1:
        return [jax.ShapeDtypeStruct((features, width), F32)]
    return [jax.ShapeDtypeStruct((count // 2, features // count, width), F32)] * 2


def weight_grad(order, lefts, rights, count, start=0, so_far=None, whole=False):
    features, width = lefts[0].shape[1], rights[0].shape[1]
    total = sum(part.shape[0] for part in lefts)
    shapes = [jax.ShapeDtypeStruct((features, width), F32)] if whole else block_shapes(count, features, width)
    outs = 0 if whole else len(shapes)
    more = [] if so_far is None else [so_far]
    vmem = len(lefts) + len(rights) + len(more)
    return pl.pallas_call(
        functools.partial(weight_grad_kernel, len(lefts), len(rights), start, bool(more), outs),
        out_shape=shapes,
        in_specs=[full(pltpu.SMEM)] + [full()] * vmem,
        out_specs=[full() if whole else full(pl.ANY)] * len(shapes),
        scratch_shapes=[
            pltpu.VMEM((total, features), BF16),
            pltpu.VMEM((total if len(rights) > 1 else 16, width), BF16),
            pltpu.VMEM((8, width) if whole else (features, width), F32),
            pltpu.SemaphoreType.DMA((count,)),
        ],
        compiler_params=pltpu.CompilerParams(vmem_limit_bytes=VMEM_LIMIT),
        cost_estimate=pl.CostEstimate(
            flops=2 * total * features * width, bytes_accessed=8 * features * width, transcendentals=0
        ),
    )(order, *lefts, *rights, *more)


def back_through(order, backs, pre, down_pieces, start):
    features = backs[0].shape[1]
    width = pre.shape[1]
    total = sum(back.shape[0] for back in backs)
    pieces = len(down_pieces)
    return pl.pallas_call(
        functools.partial(back_pre_kernel, len(backs), pieces, start),
        out_shape=jax.ShapeDtypeStruct((total, width), BF16),
        in_specs=[full(pltpu.SMEM)] + [full()] * (len(backs) + 1) + [full(pltpu.HBM)] * pieces,
        out_specs=full(),
        scratch_shapes=[
            pltpu.VMEM((total, features), BF16),
            pltpu.VMEM((features, width), BF16),
            pltpu.SemaphoreType.DMA((pieces,)),
        ],
        compiler_params=pltpu.CompilerParams(vmem_limit_bytes=VMEM_LIMIT),
        cost_estimate=pl.CostEstimate(
            flops=2 * total * features * width, bytes_accessed=8 * features * width, transcendentals=total * width
        ),
    )(order, *backs, pre, *down_pieces)


def after(value, earlier):
    return lax.optimization_barrier((value, earlier))[0]


def swap_plane(value, flip, size):
    return lax.ppermute(value, PLANE, [(spot, spot ^ flip) for spot in range(size)])


def swap_col(value, flip, size):
    return lax.ppermute(value, "col", [(spot, spot ^ flip) for spot in range(size)])


def swap_both(value, flip, plane, columns):
    pairs = []
    for spot in range(plane):
        for col in range(columns):
            pairs.append((spot * columns + col, (spot ^ flip[0]) * columns + (col ^ flip[1])))
    return lax.ppermute(value, ("dp", "row", "col"), pairs)


def chips_of_plane(even, odd, size):
    return [even] + [swap_plane((even, odd)[flip % 2], 2 * flip, size) for flip in range(1, size // 2)]


def both_cores(shards, size):
    pieces = []
    for shard in shards:
        pieces += [shard, swap_plane(shard, 1, size)]
    return pieces


def spread_col(value, size):
    return [value] + [swap_col(value, flip, size) for flip in range(1, size)]


def condition(times, embedded, offset, rows):
    half = D // 2
    places = offset + jnp.arange(rows, dtype=jnp.int32)
    low = places < half
    power = jnp.where(low, places, places - half).astype(F32)
    freqs = jnp.exp(-math.log(10000.0) * power / half)
    angle = (1000.0 * times)[:, None] * freqs[None, :]
    features = jnp.where(low[None, :], jnp.cos(angle), jnp.sin(angle))
    return jax.nn.silu(embedded + features).astype(BF16)


def modulation_part(labels, step_index, class_table, teacher_mod, student_mod, earlier, fast, plane):
    rows = teacher_mod.shape[0]
    packed = labels * 16 + step_index
    if fast:
        others = [swap_plane(packed, flip, plane) for flip in range(1, plane)]
        everyone = jnp.concatenate([packed] + others, axis=0)
    else:
        everyone = lax.all_gather(packed, PLANE, axis=0, tiled=True)
    everyone = after(everyone, earlier)
    all_labels, all_steps = everyone // 16, everyone % 16
    all_now = all_steps.astype(F32) / STEPS
    offset = lax.axis_index(PLANE) * rows
    table = lax.dynamic_slice_in_dim(class_table, offset, rows, 1)
    onehot = (all_labels[:, None] == jnp.arange(CLASSES, dtype=jnp.int32)[None, :]).astype(BF16)
    embedded = jnp.dot(onehot, table, preferred_element_type=F32)
    rows_now = condition(all_now, embedded, offset, rows)
    rows_mid = condition(all_now - 0.5 / STEPS, embedded, offset, rows)
    count = rows_now.shape[0]
    share = teacher_mod.shape[2]
    teacher_flat = teacher_mod.reshape(rows, 3 * share)
    student_flat = student_mod.reshape(rows, 3 * share)
    teacher_part = jnp.dot(
        jnp.concatenate([rows_now, rows_mid], axis=0), teacher_flat, preferred_element_type=F32
    )
    student_part = jnp.dot(rows_now, student_flat, preferred_element_type=F32)
    return jnp.concatenate([teacher_part[:count], teacher_part[count:], student_part], axis=1)


def modulation_sum(part, samples, fast, square, plane):
    if not fast:
        return lax.psum_scatter(part, PLANE, scatter_dimension=0, tiled=True)
    part = part.reshape(plane // 2, 2, samples, part.shape[1])
    pair = part[:, 0] + swap_plane(part[:, 1], 1, plane)
    share = part.shape[3] // 9

    def sent(flip):
        if not square:
            return pair[flip]
        near = pair[flip ^ 1]
        return jnp.concatenate([pair[flip], near[:, : 2 * share], near[:, 3 * share : 5 * share]], axis=1)

    own = sent(0)
    for flip in range(1, plane // 2):
        own = own + swap_plane(sent(flip), 2 * flip, plane)
    return own


def modulation_columns(own, share, columns, col):
    packed = own.reshape(-1, share)
    gathered = spread_col(packed, columns)
    ordered = []
    for place_at in range(columns):
        piece = gathered[place_at]
        for other in range(1, columns):
            piece = jnp.where(col == other, gathered[place_at ^ other], piece)
        ordered.append(piece)
    return jnp.concatenate(ordered, axis=1)


def positions(chunks, tokens):
    quarter = D // 4
    omega = 1.0 / 10000.0 ** (jnp.arange(quarter, dtype=F32) / quarter)
    side = math.isqrt(SEQ)
    span = tokens // side
    angle = jnp.arange(side, dtype=F32)[:, None] * omega[None, :]
    across = jnp.concatenate([jnp.zeros((side, D // 2), F32), jnp.sin(angle), jnp.cos(angle)], axis=1)
    grid_rows = chunks[:, None] * span + jnp.arange(span, dtype=jnp.int32)
    turn = grid_rows.astype(F32)[:, :, None] * omega
    down = jnp.concatenate(
        [jnp.sin(turn), jnp.cos(turn), jnp.zeros((chunks.shape[0], span, D // 2), F32)], axis=2
    )
    return down, across


def body(
    latents,
    labels,
    step_index,
    seeds,
    class_table,
    teacher_patch,
    teacher_mod,
    teacher_up,
    teacher_down,
    teacher_out,
    student_patch,
    student_mod,
    student_up,
    student_down,
    student_out,
):
    samples = latents.shape[0]
    plane = lax.axis_size(PLANE)
    columns = lax.axis_size("col")
    batch_total = samples * plane
    col = lax.axis_index("col")
    spot = lax.axis_index(PLANE)
    rows = teacher_up.shape[0]
    tokens = SEQ // columns
    fast = rows % 16 == 0 and plane <= 8
    count = plane if fast else 1

    order = ((jnp.arange(count, dtype=jnp.int32) ^ spot) * rows).astype(jnp.int32)

    square = fast and columns == 4 and plane >= 4
    odd_chip = (spot // 2) % 2 == 1

    def chips(even, odd=None):
        if fast:
            return chips_of_plane(even, even if odd is None else odd, plane)
        return [lax.all_gather(even, PLANE, axis=0, tiled=True)]

    def cores(shards):
        return both_cores(shards, plane) if fast else shards

    def teacher_shards(shard, abroad):
        if not square:
            return (shard,)
        return jnp.where(odd_chip, abroad, shard), jnp.where(odd_chip, shard, abroad)

    up_abroad = swap_col(teacher_up, 2, columns) if square else teacher_up
    down_abroad = swap_col(after(teacher_down, up_abroad), 2, columns) if square else teacher_down
    student_up_shards = chips(student_up)
    up_sent = teacher_shards(teacher_up, up_abroad)
    up_shards = chips(*up_sent)
    part = modulation_part(
        labels, step_index, class_table, teacher_mod, student_mod, up_sent, fast, plane
    )
    own_mods = modulation_sum(part, samples, fast, square, plane)
    mods = modulation_columns(own_mods, teacher_mod.shape[2], columns, col)
    teacher_up_pieces = cores(up_shards)
    down_shards = chips(*teacher_shards(teacher_down, down_abroad))
    teacher_down_pieces = cores(down_shards)
    student_down_shards = chips(after(student_down, own_mods))
    latents, seeds, col, step_index = after((latents, seeds, col, step_index), part)

    if square:
        members = [(0, 0), (0, 1), (2, 0), (2, 1)]
    else:
        members = [(0, flip) for flip in range(columns)]
    chunks = jnp.arange(columns, dtype=jnp.int32) ^ col
    pos = positions(chunks, tokens)
    now = step_index.astype(F32) / STEPS
    alpha, sigma = plan(now)
    alpha_mid, sigma_mid = plan(now - 0.5 / STEPS)
    alpha_end, sigma_end = plan(now - 1.0 / STEPS)
    ratio = sigma_end / sigma
    weight = jnp.maximum(alpha * alpha / (sigma * sigma), 1.0)
    push = -2.0 * sigma * weight / batch_total
    values = [alpha, sigma, alpha_mid, sigma_mid, alpha_end, sigma_end, ratio, alpha_end - ratio * alpha, push]
    lane = lax.broadcasted_iota(jnp.int32, (samples, len(values)), 1)
    coefs = jnp.zeros((samples, len(values)), F32)
    for place_at, value in enumerate(values):
        coefs = jnp.where(lane == place_at, value[:, None], coefs)
    clean = latents.reshape(samples, columns, tokens, PATCH)
    clean = jnp.take(jnp.transpose(clean, (1, 0, 3, 2)), chunks, axis=0)
    token = chunks[:, None, None, None] * tokens + jnp.arange(tokens, dtype=jnp.int32)
    places = token * PATCH + jnp.arange(PATCH, dtype=jnp.int32)[None, None, :, None]
    shaped = (1, samples, 1, 1)
    noisy = alpha.reshape(shaped) * clean + sigma.reshape(shaped) * noise_at(
        seeds.reshape(shaped), places
    )

    def share(parts, flips):
        return [parts[0]] + [
            swap_both(part, flip, plane, columns) for part, flip in zip(parts[1:], flips[1:])
        ]

    def teach(state, first_mod):
        return forward(
            order, state, teacher_patch, teacher_pos, mods, teacher_up_pieces, teacher_down_pieces,
            first_mod, False, 2 if square else 0,
        )

    student_up_pieces = cores(after(student_up_shards, down_shards))
    teacher_pos, teacher_noisy = pos, noisy
    if square:
        near = noisy[:2]
        teacher_noisy = jnp.concatenate([near, swap_plane(near, 2, plane)], axis=0)
        teacher_pos = (jnp.concatenate([pos[0][:2], pos[0][:2]], axis=0), pos[1])
    line = [(0, flip) for flip in range(columns)]
    parts = teach(teacher_noisy, 0)
    first = share(parts, members)
    student_down_pieces = cores(after(student_down_shards, parts))
    saved = forward(order, noisy, student_patch, pos, mods, student_up_pieces, student_down_pieces, 6, True)
    halfway = middle(coefs, noisy[0], teacher_patch, pos, mods, teacher_out, after(first, saved))
    half_all = jnp.stack([halfway] + [swap_both(halfway, flip, plane, columns) for flip in members[1:]], axis=0)
    early = swap_both(saved[2 % columns], line[2 % columns], plane, columns)
    student = [saved[0], early] + [
        swap_both(after(saved[spot], half_all), line[spot], plane, columns)
        for spot in range(1, columns)
        if spot != 2 % columns
    ]
    second = share(teach(half_all, 3), members)
    act, pre, hidden = saved[columns:]
    back = last(
        coefs,
        noisy[0],
        halfway,
        teacher_patch,
        student_patch,
        pos,
        mods,
        teacher_out,
        student_out,
        second,
        student,
    )
    if columns == 4:
        across = swap_col(back, 2, columns)
        beside = swap_col(back, 1, columns)
        backs = [back, beside, across, swap_col(across, 1, columns)]
    else:
        backs = spread_col(back, columns)

    def pair_sum(blocks):
        if not fast:
            return blocks[0]
        mine, other = blocks
        return mine + swap_plane(other, 1, plane)

    def chip_sum(pair):
        if not fast:
            return lax.psum_scatter(pair, PLANE, scatter_dimension=0, tiled=True)
        total = pair[0]
        for flip in range(1, plane // 2):
            total = total + swap_plane(pair[flip].astype(BF16), 2 * flip, plane).astype(F32)
        return total

    split = (columns - 1) * back.shape[0]
    (down_early,) = weight_grad(order, backs[:-1], [hidden], count, whole=True)
    pre_early = back_through(order, backs[:-1], pre, student_down_pieces, 0)
    down_blocks = weight_grad(order, after(backs[-1:], pre_early), [hidden], count, split, down_early)
    pre_late = back_through(order, backs[-1:], after(pre, down_blocks), student_down_pieces, split)
    down_pair = pair_sum(down_blocks)
    up_blocks = weight_grad(order, [after(act, down_pair)], [pre_early, pre_late], count)
    down_gradient = chip_sum(down_pair)
    up_gradient = chip_sum(pair_sum(up_blocks))
    return (up_gradient, down_gradient)


def solution(mesh):
    rows = P(("dp", "row"), "col")
    mod = P(("dp", "row"), None, "col")
    batch = P(("dp", "row"))
    placed = (
        P(("dp", "row"), None, None),
        batch,
        batch,
        batch,
        P(),
        P(),
        mod,
        rows,
        rows,
        P(),
        P(),
        mod,
        rows,
        rows,
        P(),
    )

    return jax.shard_map(body, mesh=mesh, in_specs=placed, out_specs=(rows, rows), check_vma=False)
```
